32 devices in a mesh: bl: 8 (over y, x, core), bp: 4 (over z).
Axes of the slice: x: 2, y: 2, z: 4, core: 2. Of those that a mesh axis runs over, the one named last changes fastest.
Arguments:
- inverse_cov: float32 [8, 1024, 1024], P('bl', 'bp'), may hold values from -1 to 12, as said below
- channel_keep_mask: int32 [8, 1024], P('bl'), may hold values 0 or 1
- partner_ids: int32 [8, 2], P('bl'), may hold values from -1 to 7, as said below
- band_starts: int32 [2, 64], replicated, may hold values from 0 to 384
Outputs:
- fisher: float32 [2, 64, 64], P(None, 'bp', 'bl')
The draws below stay inside these ranges and needn't reach their ends.
Inputs may be any that keep to these rules, and one draw needn't show every extreme that they name: partner_ids[i, k] is -1 for an empty slot, else the index of a baseline whose group, its index // 1, lies 1 to 4 groups after the group of baseline i, counted cyclically over the 8 groups; in every draw some baseline has all 2 slots filled. Each inverse_cov[i] is symmetric.
All inputs are finite; a program needn't handle non-finite values. No bound on the sum of `channel_keep_mask` on one device may be relied on, other than what follows from the above.
Results may differ from the reference program's by a relative error of at most 0.0003.
Values sent between devices are 32-bit elements; how exact they have to be, the bound alone decides.
A program may use at most 128 MiB of HBM per device.

```python
from functools import partial
import jax
import jax.numpy as jnp
from jax import lax

CHANNEL_COUNT = 1024
PANEL = 512
BANDPOWER_COUNT = 64
WINDOW_LENGTH = 128
PAIRS_PER_SHARD = 1
ANTENNA_PAIRS = 8
COMPANION_SEATS = 2
GROUP_REACH = 4


def draw_inverse_cov(key, part):
    seed_sequence = jax.random.split(key, 5)
    rough_estimate = jax.random.uniform(seed_sequence[0], (ANTENNA_PAIRS, CHANNEL_COUNT, CHANNEL_COUNT), jnp.float32, -1.0, 1.0)
    coupled = (rough_estimate + jnp.swapaxes(rough_estimate, 1, 2)) * (0.5 / 32.0)
    identity = jnp.eye(CHANNEL_COUNT, dtype=jnp.float32)
    diagonal_entries = jax.random.uniform(seed_sequence[1], (ANTENNA_PAIRS, CHANNEL_COUNT), jnp.float32, 1.0, 2.0)
    channel_weighting = jax.random.uniform(seed_sequence[2], (ANTENNA_PAIRS, CHANNEL_COUNT), jnp.float32, 0.5, 1.5)
    correlation_length = jnp.exp(jax.random.uniform(seed_sequence[3], (ANTENNA_PAIRS,), jnp.float32, jnp.log(CHANNEL_COUNT / 4.0), jnp.log(CHANNEL_COUNT * 1.0)))
    signal_amplitude = jax.random.uniform(seed_sequence[4], (ANTENNA_PAIRS,), jnp.float32, 0.04, 0.1)
    channel_pos = jnp.arange(CHANNEL_COUNT, dtype=jnp.float32)
    spread = jnp.abs(channel_pos[:, None] - channel_pos[None, :])
    smooth = signal_amplitude[:, None, None] * channel_weighting[:, :, None] * channel_weighting[:, None, :] * jnp.exp(-spread[None, :, :] / correlation_length[:, None, None])
    alternating = 1.0 - 2.0 * (jnp.arange(CHANNEL_COUNT, dtype=jnp.int32) % 2).astype(jnp.float32)
    parity = 0.1 * alternating[:, None] * alternating[None, :]
    matrix = coupled * (1.0 - identity) + identity * diagonal_entries[:, :, None] + smooth + parity[None, :, :]
    return matrix


def draw_partner_ids(key, part):
    seed_sequence = jax.random.split(key, 6)
    antenna_pair_sets = ANTENNA_PAIRS // PAIRS_PER_SHARD
    antenna_pair_number = jnp.arange(ANTENNA_PAIRS, dtype=jnp.int32)
    rotation_team = antenna_pair_number // PAIRS_PER_SHARD
    turn_shift = jax.random.randint(seed_sequence[0], (), 0, GROUP_REACH, dtype=jnp.int32)
    phase_bit = jax.random.randint(seed_sequence[1], (), 0, 2, dtype=jnp.int32)
    heaviest_group = jax.random.randint(seed_sequence[2], (), 0, ANTENNA_PAIRS, dtype=jnp.int32)
    additional_step = jax.random.randint(seed_sequence[3], (ANTENNA_PAIRS, COMPANION_SEATS), 0, GROUP_REACH, dtype=jnp.int32)
    team_element = jax.random.randint(seed_sequence[4], (ANTENNA_PAIRS, COMPANION_SEATS), 0, PAIRS_PER_SHARD, dtype=jnp.int32)
    keep_probability = jax.random.randint(seed_sequence[5], (ANTENNA_PAIRS, COMPANION_SEATS), 0, 10, dtype=jnp.int32)
    slot_ids = jnp.arange(COMPANION_SEATS, dtype=jnp.int32)[None, :]
    first_hop = ((rotation_team + turn_shift) % GROUP_REACH)[:, None]
    number_of_hops = 1 + jnp.where(slot_ids == 0, first_hop, additional_step)
    steady = ((rotation_team + phase_bit * GROUP_REACH) // GROUP_REACH % 2 == 0)[:, None] & (slot_ids == 0)
    filled = steady | (keep_probability < 3) | (antenna_pair_number == heaviest_group)[:, None]
    companion_pair = (rotation_team[:, None] + number_of_hops) % antenna_pair_sets * PAIRS_PER_SHARD + team_element
    return jnp.where(filled, companion_pair, -1).astype(jnp.int32)


def touch_ends(result, stream_key, low, top_value):
    shape = result.shape
    spot = [jax.random.randint(jax.random.fold_in(stream_key, axis), (), 0, shape[axis]) for axis in range(len(shape))]
    result = result.at[tuple(spot)].set(low)
    longest = shape.index(max(shape))
    spot[longest] = (spot[longest] + 1) % shape[longest]
    return result.at[tuple(spot)].set(top_value)


def setup_inputs(seed: int = 0) -> dict:
    keys = jax.random.split(jax.random.key(seed), 5)
    inverse_cov = draw_inverse_cov(jax.random.fold_in(keys[4], 71), 0)
    channel_keep_mask = touch_ends((jax.random.randint(keys[1], (ANTENNA_PAIRS, CHANNEL_COUNT), 0, 5) < 4).astype(jnp.int32), jax.random.fold_in(keys[1], 1), 0, 1)
    partner_ids = draw_partner_ids(jax.random.fold_in(keys[4], 71), 0)
    band_starts = touch_ends(jax.random.randint(keys[3], (2, BANDPOWER_COUNT), 0, PANEL - WINDOW_LENGTH + 1), jax.random.fold_in(keys[3], 1), 0, PANEL - WINDOW_LENGTH).astype(jnp.int32)
    return dict(inverse_cov=inverse_cov, channel_keep_mask=channel_keep_mask, partner_ids=partner_ids, band_starts=band_starts)


highest = lax.Precision.HIGHEST


def kernel_stack(first_band, band_count, window):
    channel_pos = jnp.arange(window, dtype=jnp.float32)
    spread = jnp.abs(channel_pos[:, None] - channel_pos[None, :])
    band_ids = first_band + jnp.arange(band_count, dtype=jnp.int32)
    length = 1.0 + (band_ids % 4).astype(jnp.float32)
    return jnp.exp(-spread[None, :, :] / length[:, None, None])


def project(panel_block, starts, kernels):
    window = kernels.shape[1]
    window_rows = jax.vmap(lambda row_start: lax.dynamic_slice_in_dim(panel_block, row_start, window, 0))(starts)
    return jnp.einsum("apq,aqc->apc", kernels, window_rows, precision=highest, preferred_element_type=jnp.float32)


def column_windows(projected, starts, window):
    def one_matrix(matrix):
        return jax.vmap(lambda column_start: lax.dynamic_slice_in_dim(matrix, column_start, window, 1))(starts)
    return jax.vmap(one_matrix)(projected)


def baseline_panels(inverse_cov, channel_keep_mask, index):
    matrix = lax.dynamic_index_in_dim(inverse_cov, index, 0, keepdims=False)
    flag_marks = lax.dynamic_index_in_dim(channel_keep_mask, index, 0, keepdims=False).astype(jnp.float32)
    halves = []
    for half_index in range(2):
        lower = half_index * PANEL
        block_part = matrix[lower:lower + PANEL, lower:lower + PANEL]
        marks_half = flag_marks[lower:lower + PANEL]
        halves.append(block_part * marks_half[:, None] * marks_half[None, :])
    return halves


def pair_fisher(own_rows, partner_rows, starts):
    def one_band(inputs):
        partner_row, band_begin = inputs
        partner_windows = column_windows(partner_row[None], starts, WINDOW_LENGTH)[0]
        own_windows = column_windows(own_rows, band_begin[None], WINDOW_LENGTH)[:, 0]
        return jnp.einsum("bpq,bqp->b", partner_windows, own_windows, precision=highest, preferred_element_type=jnp.float32)
    return lax.map(one_band, (partner_rows, starts))


def slot_fisher(inverse_cov, channel_keep_mask, band_starts, kernels, own_rows, target):
    partner_halves = baseline_panels(inverse_cov, channel_keep_mask, target)
    results = []
    for half_index in range(2):
        partner_rows = project(partner_halves[half_index], band_starts[half_index], kernels)
        results.append(pair_fisher(own_rows[half_index], partner_rows, band_starts[half_index]))
    return jnp.stack(results)


def reference(inverse_cov, channel_keep_mask, partner_ids, band_starts):
    kernels = kernel_stack(0, BANDPOWER_COUNT, WINDOW_LENGTH)

    def accumulate_fisher(index, running_totals):
        own_halves = baseline_panels(inverse_cov, channel_keep_mask, index)
        own_rows = [project(own_halves[half_index], band_starts[half_index], kernels) for half_index in range(2)]
        for slot_index in range(COMPANION_SEATS):
            target = partner_ids[index, slot_index]
            safe_target = jnp.maximum(target, 0).astype(jnp.int32)
            running_totals = running_totals + lax.cond(target >= 0, partial(slot_fisher, inverse_cov, channel_keep_mask, band_starts, kernels, own_rows, safe_target), partial(jnp.zeros, (2, BANDPOWER_COUNT, BANDPOWER_COUNT), jnp.float32))
        return running_totals

    running_totals = lax.fori_loop(0, ANTENNA_PAIRS, accumulate_fisher, jnp.zeros((2, BANDPOWER_COUNT, BANDPOWER_COUNT), jnp.float32))
    return running_totals * (1.0 / (4 * ANTENNA_PAIRS * WINDOW_LENGTH))
```

```python
from functools import partial

import jax
import jax.numpy as jnp
from jax import lax
from jax.experimental import pallas as pl
from jax.experimental.pallas import tpu as pltpu
from jax.sharding import PartitionSpec as P

WINDOW_LENGTH = 128
KINDS = 4
LANES = 128
PAD = 8
MESH = pl.DeviceIdType.MESH
NT = (((1,), (1,)), ((), ()))
NN = (((1,), (0,)), ((), ()))
F32, BF16 = jnp.float32, jnp.bfloat16


def split(value):
    high = value.astype(BF16)
    return high, (value - high.astype(F32)).astype(BF16)


def dot(left, right, dims):
    return lax.dot_general(left, right, dims, preferred_element_type=F32)


def dot3(left, right, dims):
    return dot(left[0], right[0], dims) + (dot(left[0], right[1], dims) + dot(left[1], right[0], dims))


def exact(left, right, dims):
    return lax.dot_general(left, right, dims, precision=lax.Precision.HIGHEST, preferred_element_type=F32)


def iota(shape, axis):
    return lax.broadcasted_iota(jnp.int32, shape, axis)


def column_of(row, length, offset):
    shape = (length, row.shape[1])
    spot = iota(shape, 0) + offset == iota(shape, 1)
    return jnp.sum(jnp.where(spot, row, 0.0), axis=1, keepdims=True)


def decay(gap, inverse_length):
    return jnp.exp(-jnp.abs(gap) * inverse_length)


def inverse_of(ids):
    return 1.0 / (1.0 + (ids % KINDS).astype(F32))


def flipped(index, distance):
    result, bit = index, 1
    while bit <= distance:
        if distance & bit:
            result = result + bit - 2 * bit * (index // bit % 2)
        bit *= 2
    return result


def kernel(
    sizes, cov_ref, mask_ref, partner_ref, starts_ref, out_ref,
    raw, masks, partner_row, starts,
    slices, mask_all, partner_all, rim, tail, rim_out, tail_out,
    toep, toep_low, table, table_low, spread, spread_low, box, pick, reach,
    held, boxed, leak, mixed, grown, product, tiles, landed,
    load_sem, x_sem, m_sem, p_sem, c_sem, w_sem, fin_send, fin_recv, ready,
):
    groups, owners, rows, width, bands, seats = sizes
    window = WINDOW_LENGTH
    me, level = lax.axis_index("bl"), lax.axis_index("bp")
    per_half = width // rows
    half, place = level // per_half, level % per_half
    level_other = half * per_half + (per_half - 1 - place)
    slots = per_half * groups
    count = rows // groups
    share = bands // slots
    slot = place * groups + me
    first = pl.multiple_of(place * rows, rows)
    mine = pl.ds(first, rows)
    half_columns = pl.ds(pl.multiple_of(half * width, width), width)

    starts_load = pltpu.make_async_copy(starts_ref, starts, load_sem.at[2])
    loads = [
        pltpu.make_async_copy(cov_ref.at[0, :, half_columns], raw, load_sem.at[0]),
        pltpu.make_async_copy(mask_ref, masks, load_sem.at[1]),
        pltpu.make_async_copy(partner_ref, partner_row, load_sem.at[3]),
    ]
    for load in loads:
        load.start()
    starts_load.start()
    barrier = pltpu.get_barrier_semaphore()
    for d in range(1, groups):
        pl.semaphore_signal(barrier, inc=1, device_id=(flipped(me, d), level), device_id_type=MESH)
    for d in range(1, owners):
        pl.semaphore_signal(barrier, inc=1, device_id=(me, (level + d) % owners), device_id_type=MESH)
    for load in loads:
        load.wait()
    pl.semaphore_wait(barrier, groups + owners - 2)

    def remote(source, target, sems, to, origin, device):
        return pltpu.make_async_remote_copy(
            src_ref=source, dst_ref=target, send_sem=sems.at[0, to], recv_sem=sems.at[1, origin],
            device_id=device, device_id_type=MESH,
        )

    def slice_of(g):
        return raw.at[pl.ds(pl.multiple_of(g * count, count), count)]

    order = list(range(1, groups))
    sent = []
    for d in order:
        g = flipped(me, d)
        sent.append(remote(masks, mask_all.at[me], m_sem, g, me, (g, level)))
        sent.append(remote(partner_row, partner_all.at[me], p_sem, g, me, (g, level)))
    for d in order:
        g = flipped(me, d)
        sent.append(remote(slice_of(g), slices.at[me], x_sem, g, me, (g, level)))
    for copy in sent:
        copy.start()
    for d in order:
        pl.semaphore_signal(ready, inc=1, device_id=(flipped(me, d), level), device_id_type=MESH)
    slices[me] = raw[pl.ds(pl.multiple_of(me * count, count), count), :]
    mask_all[me] = masks[...]
    partner_all[me] = partner_row[...]

    starts_load.wait()
    start_row = starts[pl.ds(half, 1), :].astype(F32)
    start = column_of(start_row, bands, 0)
    band_ids = iota((bands, 1), 0)
    inverse_length = inverse_of(band_ids)
    channel = iota((bands, width), 1).astype(F32)
    ahead = channel - start
    past = ahead - (window - 1)
    within = jnp.logical_and(ahead >= 0.0, past <= 0.0)
    rise, fall = decay(ahead, inverse_length), decay(past, inverse_length)
    ramp_rise = jnp.where(within, rise, 0.0)
    ramp_fall = jnp.where(within, fall, 0.0)
    edge_up = jnp.where(ahead < 0.0, rise, 0.0)
    edge_down = jnp.where(past > 0.0, fall, 0.0)
    mid_ids = iota((2 * KINDS, 1), 0)
    mid_channel = iota((2 * KINDS, width), 1).astype(F32) - rows
    mid_gap = jnp.where(mid_ids < KINDS, -1.0 - mid_channel, mid_channel)
    edge_mid = jnp.where(mid_gap >= 0.0, decay(mid_gap, inverse_of(mid_ids)), 0.0)
    fence_ids = iota((slots * KINDS, 1), 0)
    fence_gap = (fence_ids // KINDS * count - 1).astype(F32) - iota((slots * KINDS, width), 1).astype(F32)
    fence = jnp.where(fence_gap >= 0.0, decay(fence_gap, inverse_of(fence_ids)), 0.0)
    table[...], table_low[...] = split(
        jnp.concatenate([edge_up, edge_down, edge_mid, jnp.zeros_like(edge_mid), ramp_rise, ramp_fall], axis=0))
    ramp_at = 2 * bands + 4 * KINDS

    marks = masks[:, half_columns].astype(F32)
    panel = split(raw[...] * column_of(marks, rows, first) * marks)
    summed = dot3(split(jnp.concatenate([fence, edge_up, ramp_rise], axis=0)), panel, NT)
    fences, ups, rises = summed[:slots * KINDS], summed[slots * KINDS:slots * KINDS + bands], summed[slots * KINDS + bands:]
    rim_out[...] = jnp.zeros_like(rim_out)
    for s in range(slots):
        rim_out[s, 0:KINDS, :] = fences[s * KINDS:(s + 1) * KINDS]
        rim_out[s, KINDS:KINDS + share, :] = ups[s * share:(s + 1) * share]
        tail_out[s] = rises[s * share:(s + 1) * share]
    rim[me, :, mine] = rim_out[slot]
    tail[me, :, mine] = tail_out[slot]
    pl.semaphore_wait(ready, groups - 1)
    origin = place * groups + me

    def rim_copies(d, far):
        g = flipped(me, d)
        where, row = (level_other, per_half - 1 - place) if far else (level, place)
        to = row * groups + g
        return [
            remote(rim_out.at[to], rim.at[me, :, mine], c_sem, to, origin, (g, where)),
            remote(tail_out.at[to], tail.at[me, :, mine], w_sem, to, origin, (g, where)),
        ]

    rims = [rim_copies(d, far) for d in range(groups) for far in (False, True) if far or d]
    for kind in range(2):
        for pair in rims:
            pair[kind].start()
            sent.append(pair[kind])

    far_apart = (iota((rows, rows), 0) - iota((rows, rows), 1)).astype(F32)
    for k in range(KINDS):
        toep[k], toep_low[k] = split(decay(far_apart, 1.0 / (1 + k)))
    for k in range(KINDS):
        box[:, k * width:(k + 1) * width] = jnp.where(
            jnp.logical_and(within, band_ids % KINDS == k), 1.0, 0.0).astype(BF16)
    sides = iota((bands, 2 * bands), 1) % bands == iota((bands, 2 * bands), 0)
    box[:, KINDS * width:] = jnp.where(sides, -1.0, 0.0).astype(BF16)

    tile_b, tile_a = bands // groups, bands // owners
    span = tile_a * tile_b
    lanes = owners * span
    lane_band = iota((bands, lanes), 1) // tile_b
    lane_start = exact(start_row, (lane_band == iota((bands, lanes), 0)).astype(F32), NN)
    step_rows = KINDS * count
    row_ids = iota((step_rows, lanes), 0)
    row_channel = (row_ids % count + slot * count).astype(F32)
    row_ahead = row_channel - lane_start
    inside = jnp.logical_and(row_ahead >= 0.0, row_ahead <= window - 1.0)
    of_kind = iota((step_rows, lanes), 1) // tile_b % KINDS == row_ids // count
    pick[0:step_rows, :] = jnp.where(jnp.logical_and(inside, of_kind), 1.0, 0.0)
    rim_band = slot * share + iota((PAD, lanes), 0) - KINDS
    own_band = jnp.logical_and(iota((PAD, lanes), 1) // tile_b == rim_band, iota((PAD, lanes), 0) >= KINDS)
    pick[step_rows:, :] = jnp.where(
        jnp.logical_and(own_band, iota((PAD, lanes), 0) < KINDS + share), -1.0, 0.0)

    total = groups * count
    gap = (iota((step_rows, total), 0) % count - iota((step_rows, total), 1) % count).astype(F32)
    reach_value = decay(gap, inverse_of(iota((step_rows, total), 0) // count))
    reach[...] = jnp.where(gap > 0.0, reach_value, jnp.where(gap == 0.0, 0.5, 0.0))

    def wait_from(target, sems, origin_index, device):
        remote(target, target, sems, origin_index, origin_index, device).wait_recv()

    for d in order:
        g = flipped(me, d)
        wait_from(partner_all.at[g], p_sem, g, (g, level))
        wait_from(mask_all.at[g], m_sem, g, (g, level))

    lane_of = iota((1, total), 1) // count
    lane_pad = iota((1, groups * PAD), 1) // PAD
    seat_lane, seat_pad, seat_value = [], [], []
    for k in range(seats):
        values = [partner_all[i][:, k:k + 1] for i in range(groups)]
        seat_value.append(values)
        seat_lane.append(sum(jnp.where(lane_of == i, values[i], 0) for i in range(groups)))
        seat_pad.append(sum(jnp.where(lane_pad == i, values[i], 0) for i in range(groups)))

    def weights(j, ids, by_lane):
        found = 0.0
        for k in range(seats):
            found = found + jnp.where(ids == seat_value[k][j], 1.0, 0.0) + jnp.where(by_lane[k] == j, 1.0, 0.0)
        return found

    blend_rows = []
    slot_lane = iota((PAD, groups * PAD), 1) % PAD == iota((PAD, groups * PAD), 0)
    for j in range(groups):
        spread[j], spread_low[j] = split(reach[...] * weights(j, lane_of, seat_lane))
        blend_rows.append(jnp.where(slot_lane, weights(j, lane_pad, seat_pad), 0.0))
    blend = jnp.concatenate(blend_rows, axis=0).astype(BF16)

    lane_f = iota((1, rows), 1).astype(F32)

    def filtered(value):
        n = value.shape[0]
        found = dot3(split(value), (table[0:ramp_at, :], table_low[0:ramp_at, :]), NT)
        stacked = split(jnp.concatenate([value[:, 0:rows], value[:, rows:]], axis=0))
        both = jnp.concatenate(stacked, axis=0)
        results = []
        for k in range(KINDS):
            r = dot(both, toep[k], NN)
            r = r[0:2 * n] + r[2 * n:] + dot(stacked[0], toep_low[k], NN)
            up = found[:, 2 * bands + k:2 * bands + k + 1]
            down = found[:, 2 * bands + KINDS + k:2 * bands + KINDS + k + 1]
            left = r[0:n] + down * jnp.exp((rows - lane_f) * (-1.0 / (1 + k)))
            right = r[n:] + up * jnp.exp((lane_f + 1.0) * (-1.0 / (1 + k)))
            results.append((left, right))
        return found[:, 0:2 * bands], results

    def ramped(value):
        return dot3(split(value), (table[ramp_at:, :], table_low[ramp_at:, :]), NT)

    in_lane = slot * count
    lane_base = pl.multiple_of(half * width + in_lane // LANES * LANES, LANES)
    lane_offset = in_lane % LANES

    def absorb(j):
        column_marks = mask_all[j, :, half_columns].astype(F32)
        near_marks = mask_all[j, :, pl.ds(lane_base, LANES)].astype(F32)
        value = slices[j] * column_of(near_marks, count, lane_offset) * column_marks
        held[j, :, 0:width] = value
        edges, results = filtered(value)
        leak[j] = edges
        for k in range(KINDS):
            boxed[k, j, :, 0:rows] = results[k][0]
            boxed[k, j, :, rows:] = results[k][1]
        held[j, :, width:] = ramped(value)

    absorb(me)
    for d in order:
        g = flipped(me, d)
        wait_from(slices.at[g], x_sem, g, (g, level))
        absorb(g)

    for d in range(groups):
        g = flipped(me, d)
        if d:
            wait_from(rim.at[g, :, mine], c_sem, place * groups + g, (g, level))
        other = pl.ds(pl.multiple_of(width - rows - first, rows), rows)
        wait_from(rim.at[g, :, other], c_sem, (per_half - 1 - place) * groups + g, (g, level_other))
    rims_in = jnp.reshape(rim[...], (groups * PAD, width))
    rims_in = jnp.concatenate([rims_in, ramped(rims_in)], axis=1)
    high, low = split(rims_in)
    mixed[...] = dot(blend, high, NN) + dot(blend, low, NN)

    held_split = split(jnp.reshape(held[...], (total, width + 2 * bands)))
    rank = (iota((count, 1), 0) + 1).astype(F32)
    for j in range(groups):
        found = dot3((spread[j], spread_low[j]), held_split, NN)
        for m in range(KINDS):
            at = slice(m * count, (m + 1) * count)
            carry = mixed[j * PAD + m:j * PAD + m + 1, :]
            grown[j, at, :] = found[at] + jnp.exp(rank * (-1.0 / (1 + m))) * carry

    for d in range(groups):
        g = flipped(me, d)
        if d:
            wait_from(tail.at[g, :, mine], w_sem, place * groups + g, (g, level))
        other = pl.ds(pl.multiple_of(width - rows - first, rows), rows)
        wait_from(tail.at[g, :, other], w_sem, (per_half - 1 - place) * groups + g, (g, level_other))
    blank, spare = jnp.zeros((KINDS, width), F32), jnp.zeros((KINDS - share, width), F32)
    tails = []
    for j in range(groups):
        tails += [blank, tail[j]] + ([spare] if share < KINDS else [])
    tail_edges, tail_results = filtered(jnp.concatenate(tails, axis=0))

    for k in range(KINDS):
        line = jnp.concatenate(tail_results[k], axis=1)
        product[step_rows:, k * width:(k + 1) * width] = sum(
            mixed[j * PAD:(j + 1) * PAD, 0:width] * line[j * PAD:(j + 1) * PAD] for j in range(groups))
    product[step_rows:, KINDS * width:] = sum(
        mixed[j * PAD:(j + 1) * PAD, width:] * tail_edges[j * PAD:(j + 1) * PAD] for j in range(groups))

    for pb in range(count // 8):
        here = slice(pb * 8, pb * 8 + 8)
        for m in range(KINDS):
            rows_at = slice(m * count + pb * 8, m * count + pb * 8 + 8)
            product[rows_at, KINDS * width:] = sum(
                grown[j, rows_at, width:] * leak[j, here, :] for j in range(groups))
        for qb in range(width // LANES):
            cols = slice(qb * LANES, (qb + 1) * LANES)
            sums = [[0.0] * KINDS for _ in range(KINDS)]
            for j in range(groups):
                lefts = [grown[j, m * count + pb * 8:m * count + pb * 8 + 8, cols] for m in range(KINDS)]
                rights = [boxed[k, j, here, cols] for k in range(KINDS)]
                for m in range(KINDS):
                    for k in range(KINDS):
                        term = lefts[m] * rights[k]
                        sums[m][k] = term if j == 0 else sums[m][k] + term
            for m in range(KINDS):
                for k in range(KINDS):
                    product[m * count + pb * 8:m * count + pb * 8 + 8,
                            k * width + qb * LANES:k * width + (qb + 1) * LANES] = sums[m][k]

    high, low = split(product[...])
    turned = split(dot(box[...], high, NT) + dot(box[...], low, NT))
    picks = pick[...].astype(BF16)
    fisher = (dot(turned[0], picks, NN) + dot(turned[1], picks, NN)) * (1.0 / (4 * groups * window))
    kept = jnp.where(iota((bands, lanes), 0) % tile_b == iota((bands, lanes), 1) % tile_b, fisher, 0.0)
    for g in range(groups):
        packed = jnp.sum(kept[g * tile_b:(g + 1) * tile_b], axis=0, keepdims=True)
        for z in range(owners):
            tiles[z * groups + g] = packed[:, z * span:(z + 1) * span]

    everyone = groups * owners
    here = level * groups + me
    landed[pl.ds(here, 1)] = tiles[pl.ds(here, 1)]
    for d in range(1, everyone):
        peer = (here + d) % everyone
        copy = pltpu.make_async_remote_copy(
            src_ref=tiles.at[peer], dst_ref=landed.at[here], send_sem=fin_send.at[peer], recv_sem=fin_recv.at[here],
            device_id=(peer % groups, peer // groups), device_id_type=MESH,
        )
        copy.start()
        sent.append(copy)
    for d in range(1, everyone):
        peer = (here + d) % everyone
        pltpu.make_async_remote_copy(
            src_ref=tiles.at[peer], dst_ref=landed.at[peer], send_sem=fin_send.at[peer], recv_sem=fin_recv.at[peer],
            device_id=(peer % groups, peer // groups), device_id_type=MESH,
        ).wait_recv()
    keep = iota((tile_a, span), 0) == iota((tile_a, span), 1) // tile_b
    spots = (iota((span, tile_b), 0) % tile_b == iota((span, tile_b), 1)).astype(F32)
    for h in range(2):
        row = jnp.sum(landed[h * everyone // 2:(h + 1) * everyone // 2], axis=0)
        out_ref[h] = exact(jnp.where(keep, row, 0.0), spots, NN)
    for copy in sent:
        copy.wait_send()


def solution(mesh):
    groups, owners = mesh.shape["bl"], mesh.shape["bp"]

    def body(inverse_cov, channel_keep_mask, partner_ids, band_starts):
        number, rows, channels = inverse_cov.shape
        width, bands, seats = channels // 2, band_starts.shape[1], partner_ids.shape[1]
        per_half = width // rows
        slots = per_half * groups
        count, share = rows // groups, bands // slots
        assert number == 1 and per_half == 2 and count % 8 == 0 and 1 <= share <= KINDS
        tile_b, tile_a = bands // groups, bands // owners
        wide = width + 2 * bands
        step_rows = KINDS * count
        everyone = groups * owners
        dma = pltpu.SemaphoreType.DMA

        def vmem(shape, dtype=F32):
            return pltpu.VMEM(shape, dtype)

        return pl.pallas_call(
            partial(kernel, (groups, owners, rows, width, bands, seats)),
            name="fisher",
            out_shape=jax.ShapeDtypeStruct((2, tile_a, tile_b), F32),
            in_specs=[pl.BlockSpec(memory_space=pltpu.HBM)] * 4,
            out_specs=pl.BlockSpec(memory_space=pltpu.VMEM),
            scratch_shapes=[
                vmem((rows, width)),
                vmem(channel_keep_mask.shape, jnp.int32),
                vmem(partner_ids.shape, jnp.int32),
                vmem(band_starts.shape, jnp.int32),
                vmem((groups, count, width)),
                vmem((groups, 1, channels), jnp.int32),
                vmem((groups, 1, seats), jnp.int32),
                vmem((groups, PAD, width)),
                vmem((groups, share, width)),
                vmem((slots, PAD, rows)),
                vmem((slots, share, rows)),
                vmem((KINDS, rows, rows), BF16),
                vmem((KINDS, rows, rows), BF16),
                vmem((4 * bands + 4 * KINDS, width), BF16),
                vmem((4 * bands + 4 * KINDS, width), BF16),
                vmem((groups, step_rows, rows), BF16),
                vmem((groups, step_rows, rows), BF16),
                vmem((bands, KINDS * width + 2 * bands), BF16),
                vmem((step_rows + PAD, bands * tile_b)),
                vmem((step_rows, rows)),
                vmem((groups, count, wide)),
                vmem((KINDS, groups, count, width)),
                vmem((groups, count, 2 * bands)),
                vmem((groups * PAD, wide)),
                vmem((groups, step_rows, wide)),
                vmem((step_rows + PAD, KINDS * width + 2 * bands)),
                vmem((everyone, 1, tile_a * tile_b)),
                vmem((everyone, 1, tile_a * tile_b)),
                dma((4,)), dma((2, groups)), dma((2, groups)), dma((2, groups)), dma((2, slots)), dma((2, slots)),
                dma((everyone,)), dma((everyone,)), pltpu.SemaphoreType.REGULAR,
            ],
            compiler_params=pltpu.CompilerParams(
                collective_id=0, has_side_effects=True, vmem_limit_bytes=67043328
            ),
        )(inverse_cov, channel_keep_mask, partner_ids, band_starts)

    placed = (P("bl", "bp", None), P("bl", None), P("bl", None), P())
    return jax.shard_map(body, mesh=mesh, in_specs=placed, out_specs=P(None, "bp", "bl"), check_vma=False)
```

```python
from functools import partial

import jax
import jax.numpy as jnp
from jax import lax
from jax.experimental import pallas as pl
from jax.experimental.pallas import tpu as pltpu
from jax.sharding import PartitionSpec as P

WINDOW_LENGTH = 128
KINDS = 4
LANES = 128
PAD = 8
LATE = 2
MESH = pl.DeviceIdType.MESH
NT = (((1,), (1,)), ((), ()))
NN = (((1,), (0,)), ((), ()))
F32, BF16 = jnp.float32, jnp.bfloat16


def split(value):
    high = value.astype(BF16)
    return high, (value - high.astype(F32)).astype(BF16)


def dot(left, right, dims):
    return lax.dot_general(left, right, dims, preferred_element_type=F32)


def dot3(left, right, dims):
    return dot(left[0], right[0], dims) + (dot(left[0], right[1], dims) + dot(left[1], right[0], dims))


def exact(left, right, dims):
    return lax.dot_general(left, right, dims, precision=lax.Precision.HIGHEST, preferred_element_type=F32)


def iota(shape, axis):
    return lax.broadcasted_iota(jnp.int32, shape, axis)


def column_of(row, length, offset):
    shape = (length, row.shape[1])
    spot = iota(shape, 0) + offset == iota(shape, 1)
    return jnp.sum(jnp.where(spot, row, 0.0), axis=1, keepdims=True)


def decay(gap, inverse_length):
    return jnp.exp(-jnp.abs(gap) * inverse_length)


def inverse_of(ids):
    return 1.0 / (1.0 + (ids % KINDS).astype(F32))


def flipped(index, distance):
    result, bit = index, 1
    while bit <= distance:
        if distance & bit:
            result = result + bit - 2 * bit * (index // bit % 2)
        bit *= 2
    return result


def ordered(groups):
    bits = (groups // 2).bit_length() - 1
    far = [d for d in range(1, groups) if bin(d // 2).count("1") == bits]
    direct = [d for d in range(2, groups) if d not in far]
    late = direct[1::2] if len(direct) == 2 * LATE else direct[-LATE:]
    return [d for d in direct if d not in late], far, late


def kernel(
    sizes, cov_ref, mask_ref, partner_ref, starts_ref, out_ref,
    raw, masks, partner_row, starts,
    slices, mask_all, partner_all, rim, rim_out,
    toep, toep_low, table, table_low, spread, spread_low, box, pick,
    held, boxed, leak, blended, mixed, summits, grown, product, tiles, landed,
    load_sem, x_sem, m_sem, p_sem, c_sem, fin_sem, ready, ready_levels,
):
    groups, owners, rows, width, bands, seats = sizes
    window = WINDOW_LENGTH
    me, level = lax.axis_index("bl"), lax.axis_index("bp")
    per_half = width // rows
    half, place = level // per_half, level % per_half
    slots = per_half * groups
    count = rows // groups
    share = bands // slots
    slot = place * groups + me
    first = pl.multiple_of(place * rows, rows)
    mine = pl.ds(first, rows)
    other = pl.ds(pl.multiple_of(width - rows - first, rows), rows)
    half_columns = pl.ds(pl.multiple_of(half * width, width), width)
    early, far, late = ordered(groups)
    arrivals = [0, 1] + far + early + late
    seat_of = {d: n for n, d in enumerate(arrivals)}
    others = far + early + late + [1]
    fixed = groups - LATE
    peers = {d: flipped(me, d) for d in range(groups)}
    levels = {dz: flipped(level, dz) for dz in range(owners)}
    below, above = level > 0, level < owners - 1
    neighbours = below.astype(jnp.int32) + above.astype(jnp.int32)

    starts_load = pltpu.make_async_copy(starts_ref, starts, load_sem.at[2])
    loads = [
        pltpu.make_async_copy(cov_ref.at[0, :, half_columns], raw, load_sem.at[0]),
        pltpu.make_async_copy(mask_ref, masks, load_sem.at[1]),
        pltpu.make_async_copy(partner_ref, partner_row, load_sem.at[3]),
    ]
    starts_load.start()
    for load in loads:
        load.start()

    def tell(semaphore, device):
        pl.semaphore_signal(semaphore, inc=1, device_id=device, device_id_type=MESH)

    def tell_levels(semaphore):
        @pl.when(below)
        def _():
            tell(semaphore, (me, level - 1))

        @pl.when(above)
        def _():
            tell(semaphore, (me, level + 1))

    barrier = pltpu.get_barrier_semaphore()
    for d in others:
        tell(barrier, (peers[d], level))
    tell_levels(barrier)

    def remote(source, target, sems, n, device):
        return pltpu.make_async_remote_copy(
            src_ref=source, dst_ref=target, send_sem=sems.at[0, n], recv_sem=sems.at[1, n],
            device_id=device, device_id_type=MESH,
        )

    sent = []

    def send(copy):
        copy.start()
        sent.append(copy)

    def send_marks(d):
        n = seat_of[d]
        send(remote(partner_row, partner_all.at[n], p_sem, n, (peers[d], level)))
        send(remote(masks, mask_all.at[n], m_sem, n, (peers[d], level)))

    def send_slice(d):
        n, g = seat_of[d], peers[d]
        send(remote(raw.at[pl.ds(pl.multiple_of(g * count, count), count)], slices.at[n], x_sem, n, (g, level)))

    def send_rim(d, across):
        n, g = seat_of[d], peers[d]
        row = per_half - 1 - place if across else place
        send(remote(
            rim_out.at[row * groups + g], rim.at[n, :, mine], c_sem, across * groups + n, (g, levels[across])))

    def landing(target, sems, n, device):
        remote(target, target, sems, n, device).wait_recv()

    starts_load.wait()
    start_row = starts[pl.ds(half, 1), :].astype(F32)
    start = column_of(start_row, bands, 0)
    band_ids = iota((bands, 1), 0)
    inverse_length = inverse_of(band_ids)
    channel = iota((bands, width), 1).astype(F32)
    ahead = channel - start
    within = jnp.logical_and(ahead >= 0.0, ahead <= window - 1.0)
    rise = decay(ahead, inverse_length)
    fence_ids = iota((slots * KINDS, 1), 0)
    fence_gap = (fence_ids // KINDS * count - 1).astype(F32) - iota((slots * KINDS, width), 1).astype(F32)
    fence = jnp.where(fence_gap >= 0.0, decay(fence_gap, inverse_of(fence_ids)), 0.0)
    sources = split(jnp.concatenate(
        [fence, jnp.where(ahead < 0.0, rise, 0.0), jnp.where(within, rise, 0.0)], axis=0))

    for load in loads:
        load.wait()
    pl.semaphore_wait(barrier, groups - 1 + neighbours)
    tell_levels(ready_levels)
    for d in others:
        send_marks(d)
    for d in others:
        send_slice(d)
    slices[0] = raw[pl.ds(pl.multiple_of(me * count, count), count), :]
    mask_all[0] = masks[...]
    partner_all[0] = partner_row[...]

    marks = masks[:, half_columns].astype(F32)
    panel = split(raw[...] * column_of(marks, rows, first) * marks)
    summed = dot3(sources, panel, NT)
    fences, ups, rises = summed[:slots * KINDS], summed[slots * KINDS:slots * KINDS + bands], summed[slots * KINDS + bands:]
    if share < KINDS:
        rim_out[...] = jnp.zeros_like(rim_out)
    for s in range(slots):
        rim_out[s, 0:KINDS, :] = fences[s * KINDS:(s + 1) * KINDS]
        rim_out[s, KINDS:KINDS + share, :] = ups[s * share:(s + 1) * share]
        rim_out[s, PAD:PAD + share, :] = rises[s * share:(s + 1) * share]
    rim[0, :, mine] = rim_out[slot]
    def ladder(shape, axis):
        return iota(shape, axis).astype(F32)

    twice = jnp.concatenate([start_row, start_row], axis=1)
    pair_ids = iota((1, 2 * bands), 1)
    is_second = iota((width, 2 * bands), 1) >= bands
    pair_inverse = inverse_of(pair_ids)
    climb = ladder((width, 2 * bands), 0) - twice
    drop = climb - (window - 1.0)
    gap = jnp.where(is_second, drop, climb)
    fade = decay(gap, pair_inverse)
    inner = jnp.logical_and(climb >= 0.0, drop <= 0.0)
    outer = jnp.where(is_second, gap, -gap) > 0.0
    mid_ids = iota((1, LANES), 1)
    mid_channel = ladder((width, LANES), 0) - rows
    mid_lane = iota((width, LANES), 1)
    mid_gap = jnp.where(mid_lane < KINDS, -1.0 - mid_channel, mid_channel)
    mid_kept = jnp.logical_and(mid_gap >= 0.0, mid_lane < 2 * KINDS)
    table[...], table_low[...] = split(jnp.concatenate([
        jnp.where(outer, fade, 0.0), jnp.where(inner, fade, 0.0),
        jnp.where(mid_kept, decay(mid_gap, inverse_of(mid_ids)), 0.0)], axis=1))
    far_apart = (iota((rows, rows), 0) - iota((rows, rows), 1)).astype(F32)
    for k in range(KINDS):
        toep[k], toep_low[k] = split(decay(far_apart, 1.0 / (1 + k)))

    pl.semaphore_wait(ready_levels, neighbours)
    for d in range(1, groups):
        tell(ready, (peers[d], level))
    for d in others:
        send_rim(d, 0)

    lane_f = iota((1, rows), 1).astype(F32)
    wide = width + 2 * bands

    def filtered(value):
        n = value.shape[0]
        found = dot3(split(value), (table[...], table_low[...]), NN)
        stacked = split(jnp.concatenate([value[:, 0:rows], value[:, rows:]], axis=0))
        both = jnp.concatenate(stacked, axis=0)
        results = []
        for k in range(KINDS):
            r = dot(both, toep[k], NN)
            r = r[0:2 * n] + r[2 * n:] + dot(stacked[0], toep_low[k], NN)
            up = found[:, 4 * bands + k:4 * bands + k + 1]
            down = found[:, 4 * bands + KINDS + k:4 * bands + KINDS + k + 1]
            left = r[0:n] + down * jnp.exp((rows - lane_f) * (-1.0 / (1 + k)))
            right = r[n:] + up * jnp.exp((lane_f + 1.0) * (-1.0 / (1 + k)))
            results.append((left, right))
        return found[:, 0:2 * bands], found[:, 2 * bands:4 * bands], results

    in_lane = slot * count
    lane_base = pl.multiple_of(half * width + in_lane // LANES * LANES, LANES)
    lane_offset = in_lane % LANES

    def absorb(members):
        parts = []
        for n in members:
            near_marks = mask_all[n, :, pl.ds(lane_base, LANES)].astype(F32)
            part = slices[n] * column_of(near_marks, count, lane_offset) * mask_all[n, :, half_columns].astype(F32)
            held[n, :, 0:width] = part
            parts.append(part)
        edges, ramps, results = filtered(jnp.concatenate(parts, axis=0))
        for i, n in enumerate(members):
            at = slice(i * count, (i + 1) * count)
            leak[n] = edges[at]
            for k in range(KINDS):
                boxed[k, n, :, 0:rows] = results[k][0][at]
                boxed[k, n, :, rows:] = results[k][1][at]
            held[n, :, width:] = ramps[at]

    def take(n):
        device = (peers[arrivals[n]], level)
        landing(mask_all.at[n], m_sem, n, device)
        landing(slices.at[n], x_sem, n, device)

    take(1)
    absorb([0, 1])
    for k in range(KINDS):
        box[:, k * width:(k + 1) * width] = jnp.where(
            jnp.logical_and(within, band_ids % KINDS == k), 1.0, 0.0).astype(BF16)
    sides = iota((bands, 2 * bands), 1) % bands == iota((bands, 2 * bands), 0)
    box[:, KINDS * width:] = jnp.where(sides, -1.0, 0.0).astype(BF16)

    tile_b, tile_a = bands // groups, bands // owners
    span = tile_a * tile_b
    lanes = owners * span
    lane_band = iota((bands, lanes), 1) // tile_b
    lane_start = exact(start_row, (lane_band == iota((bands, lanes), 0)).astype(F32), NN)
    step_rows = KINDS * count
    row_ids = iota((step_rows, lanes), 0)
    row_ahead = (row_ids % count + slot * count).astype(F32) - lane_start
    inside = jnp.logical_and(row_ahead >= 0.0, row_ahead <= window - 1.0)
    of_kind = iota((step_rows, lanes), 1) // tile_b % KINDS == row_ids // count
    pick[0:step_rows, :] = jnp.where(jnp.logical_and(inside, of_kind), 1.0, 0.0)
    rim_row = iota((PAD, lanes), 0)
    own_band = jnp.logical_and(iota((PAD, lanes), 1) // tile_b == slot * share + rim_row - KINDS, rim_row >= KINDS)
    pick[step_rows:, :] = jnp.where(jnp.logical_and(own_band, rim_row < KINDS + share), -1.0, 0.0)

    pl.semaphore_wait(ready, groups - 1)
    for d in others + [0]:
        send_rim(d, 1)

    for n in range(1, groups):
        landing(partner_all.at[n], p_sem, n, (peers[arrivals[n]], level))
    names = [peers[d] for d in arrivals]
    total = fixed * count
    lane_of, lane_pad = iota((1, total), 1) // count, iota((1, groups * PAD), 1) // PAD
    chosen = [[partner_all[n][:, k:k + 1] for n in range(groups)] for k in range(seats)]

    def along(lane, values):
        found = jnp.zeros_like(lane)
        for n, value in enumerate(values):
            found = jnp.where(lane == n, value, found)
        return found

    named_lane, named_pad = along(lane_of, names[:fixed]), along(lane_pad, names)
    chosen_lane = [along(lane_of, chosen[k][:fixed]) for k in range(seats)]
    chosen_pad = [along(lane_pad, chosen[k]) for k in range(seats)]

    def weights(n, named, by_lane):
        found = 0.0
        for k in range(seats):
            found = found + jnp.where(named == chosen[k][n], 1.0, 0.0) + jnp.where(by_lane[k] == names[n], 1.0, 0.0)
        return found

    def weight(n, i):
        found = 0.0
        for k in range(seats):
            found = found + jnp.where(chosen[k][n] == names[i], 1.0, 0.0) + jnp.where(chosen[k][i] == names[n], 1.0, 0.0)
        return found

    step_gap = (iota((step_rows, total), 0) % count - iota((step_rows, total), 1) % count).astype(F32)
    reach = decay(step_gap, inverse_of(iota((step_rows, total), 0) // count))
    reach = jnp.where(step_gap > 0.0, reach, jnp.where(step_gap == 0.0, 0.5, 0.0))
    blend_rows = []
    pad_row = iota((PAD, groups * PAD), 0)
    slot_lane = jnp.logical_and(
        iota((PAD, groups * PAD), 1) % PAD == pad_row,
        jnp.logical_or(pad_row >= KINDS, iota((PAD, groups * PAD), 1) // PAD < fixed))
    for n in range(groups):
        spread[n], spread_low[n] = split(reach * weights(n, named_lane, chosen_lane))
        blend_rows.append(jnp.where(slot_lane, weights(n, named_pad, chosen_pad), 0.0))
    blend = jnp.concatenate(blend_rows, axis=0).astype(BF16)
    reach_one = split(reach[:, 0:count])

    for n in range(2, fixed, 2):
        for i in (n, n + 1):
            take(i)
        absorb([n, n + 1])

    held_split = split(jnp.reshape(held[0:fixed], (total, wide)))
    for n in range(groups):
        grown[n] = dot3((spread[n], spread_low[n]), held_split, NN)

    members = list(range(fixed, groups))
    for t in range(LATE):
        factors = [weight(fixed + t, n) for n in range(fixed)]
        leak[groups + t] = sum(factors[n] * leak[n] for n in range(fixed))
        for k in range(KINDS):
            blended[k, t] = sum(factors[n] * boxed[k, n] for n in range(fixed))
    for n in members:
        take(n)
    absorb(members)
    for t in range(LATE):
        n = fixed + t
        grown[groups + t] = dot3(reach_one, split(held[n]), NN)
        mutual = weight(n, fixed + 1 - t)
        leak[groups + t] = leak[groups + t] + mutual * leak[fixed + 1 - t]
        for k in range(KINDS):
            blended[k, t] = blended[k, t] + mutual * boxed[k, fixed + 1 - t]

    for copy in sent:
        copy.wait_send()
    sent.clear()
    for n in range(groups):
        d = arrivals[n]
        if d:
            landing(rim.at[n, :, mine], c_sem, n, (peers[d], level))
        landing(rim.at[n, :, other], c_sem, groups + n, (peers[d], levels[1]))
    blank = jnp.zeros((KINDS, width), F32)
    tops, tails = [], []
    for n in range(groups):
        tops.append(rim[n, 0:PAD, :])
        tails += [blank, rim[n, PAD:PAD + share, :]]
        if share < KINDS:
            tails.append(jnp.zeros((KINDS - share, width), F32))
    tops = jnp.concatenate(tops, axis=0)
    tail_edges, _, tail_results = filtered(jnp.concatenate(tails, axis=0))
    tops = jnp.concatenate([tops, dot3(split(tops), (table[:, 2 * bands:4 * bands], table_low[:, 2 * bands:4 * bands]), NN)], axis=1)
    summits[...] = tops
    high, low = split(tops)
    mixed[...] = dot(blend, high, NN) + dot(blend, low, NN)
    rank = (iota((count, 1), 0) + 1).astype(F32)
    fades = [jnp.exp(rank * (-1.0 / (1 + m))) for m in range(KINDS)]
    for k in range(KINDS):
        line = jnp.concatenate(tail_results[k], axis=1)
        product[step_rows:, k * width:(k + 1) * width] = sum(
            mixed[n * PAD:(n + 1) * PAD, 0:width] * line[n * PAD:(n + 1) * PAD] for n in range(groups))
    product[step_rows:, KINDS * width:] = sum(
        mixed[n * PAD:(n + 1) * PAD, width:] * tail_edges[n * PAD:(n + 1) * PAD] for n in range(groups))

    def gather(terms):
        for pb in range(count // 8):
            here = slice(pb * 8, pb * 8 + 8)
            spots = [slice(m * count + pb * 8, m * count + pb * 8 + 8) for m in range(KINDS)]
            for m in range(KINDS):
                found = sum((grown[n, spots[m], width:] + fades[m][here] * carry(m)[:, width:]) * edge[here, :] for n, edge, _, carry in terms)
                at = (spots[m], slice(KINDS * width, wide + (KINDS - 1) * width))
                product[at] = found
            for qb in range(width // LANES):
                cols = slice(qb * LANES, (qb + 1) * LANES)
                sums = [[None] * KINDS for _ in range(KINDS)]
                for n, _, box_ref, carry in terms:
                    lefts = [grown[n, spots[m], cols] + fades[m][here] * carry(m)[:, cols] for m in range(KINDS)]
                    rights = [box_ref(k)[here, cols] for k in range(KINDS)]
                    for m in range(KINDS):
                        for k in range(KINDS):
                            term = lefts[m] * rights[k]
                            sums[m][k] = term if sums[m][k] is None else sums[m][k] + term
                for m in range(KINDS):
                    for k in range(KINDS):
                        at = (spots[m], slice(k * width + qb * LANES, k * width + (qb + 1) * LANES))
                        product[at] = sums[m][k]

    def mixed_carry(n, m):
        return mixed.at[n * PAD + m:n * PAD + m + 1, :]

    def own_carry(n, m):
        return summits.at[n * PAD + m:n * PAD + m + 1, :]

    terms = [(n, leak.at[n], partial(lambda n, k: boxed.at[k, n], n), partial(mixed_carry, n)) for n in range(groups)]
    terms += [
        (groups + t, leak.at[groups + t], partial(lambda t, k: blended.at[k, t], t), partial(own_carry, fixed + t))
        for t in range(LATE)
    ]
    gather(terms)

    high, low = split(product[...])
    turned = split(dot(box[...], high, NT) + dot(box[...], low, NT))
    picks = pick[...].astype(BF16)
    fisher = (dot(turned[0], picks, NN) + dot(turned[1], picks, NN)) * (1.0 / (4 * groups * window))
    kept = jnp.where(iota((bands, lanes), 0) % tile_b == iota((bands, lanes), 1) % tile_b, fisher, 0.0)
    for g in range(groups):
        packed = jnp.sum(kept[g * tile_b:(g + 1) * tile_b], axis=0, keepdims=True)
        for z in range(owners):
            tiles[z * groups + g] = packed[:, z * span:(z + 1) * span]

    landed[0] = tiles[level * groups + me]
    finals = []
    for dz in reversed(range(owners)):
        for d in others + [0]:
            if dz or d:
                n = dz * groups + d
                copy = remote(tiles.at[levels[dz] * groups + peers[d]], landed.at[n], fin_sem, n, (peers[d], levels[dz]))
                send(copy)
                finals.append(copy)
    for copy in sent:
        copy.wait_send()
    for copy in finals:
        copy.wait_recv()
    for side in range(2):
        part = landed[side * per_half * groups:(side + 1) * per_half * groups]
        out_ref[pl.ds(half + side - 2 * side * half, 1), :] = jnp.sum(part, axis=0)


def solution(mesh):
    groups, owners = mesh.shape["bl"], mesh.shape["bp"]

    def body(inverse_cov, channel_keep_mask, partner_ids, band_starts):
        number, rows, channels = inverse_cov.shape
        width, bands, seats = channels // 2, band_starts.shape[1], partner_ids.shape[1]
        per_half = width // rows
        slots = per_half * groups
        count, share = rows // groups, bands // slots
        assert number == 1 and per_half == 2 and owners == 4 and count % 8 == 0 and 1 <= share <= KINDS
        tile_b, tile_a = bands // groups, bands // owners
        wide = width + 2 * bands
        step_rows = KINDS * count
        everyone = groups * owners
        dma = pltpu.SemaphoreType.DMA
        regular = pltpu.SemaphoreType.REGULAR

        def vmem(shape, dtype=F32):
            return pltpu.VMEM(shape, dtype)

        found = pl.pallas_call(
            partial(kernel, (groups, owners, rows, width, bands, seats)),
            name="fisher",
            out_shape=jax.ShapeDtypeStruct((2, tile_a * tile_b), F32),
            in_specs=[pl.BlockSpec(memory_space=pltpu.HBM)] * 4,
            out_specs=pl.BlockSpec(memory_space=pltpu.VMEM),
            scratch_shapes=[
                vmem((rows, width)),
                vmem(channel_keep_mask.shape, jnp.int32),
                vmem(partner_ids.shape, jnp.int32),
                vmem(band_starts.shape, jnp.int32),
                vmem((groups, count, width)),
                vmem((groups, 1, channels), jnp.int32),
                vmem((groups, 1, seats), jnp.int32),
                vmem((groups, PAD + share, width)),
                vmem((slots, PAD + share, rows)),
                vmem((KINDS, rows, rows), BF16),
                vmem((KINDS, rows, rows), BF16),
                vmem((width, 4 * bands + LANES), BF16),
                vmem((width, 4 * bands + LANES), BF16),
                vmem((groups, step_rows, (groups - LATE) * count), BF16),
                vmem((groups, step_rows, (groups - LATE) * count), BF16),
                vmem((bands, KINDS * width + 2 * bands), BF16),
                vmem((step_rows + PAD, bands * tile_b)),
                vmem((groups, count, wide)),
                vmem((KINDS, groups, count, width)),
                vmem((groups + LATE, count, 2 * bands)),
                vmem((KINDS, LATE, count, width)),
                vmem((groups * PAD, wide)),
                vmem((groups * PAD, wide)),
                vmem((groups + LATE, step_rows, wide)),
                vmem((step_rows + PAD, KINDS * width + 2 * bands)),
                vmem((everyone, 1, tile_a * tile_b)),
                vmem((everyone, 1, tile_a * tile_b)),
                dma((4,)), dma((2, groups)), dma((2, groups)), dma((2, groups)), dma((2, per_half * groups)),
                dma((2, everyone)), regular, regular,
            ],
            compiler_params=pltpu.CompilerParams(
                collective_id=0, has_side_effects=True, vmem_limit_bytes=67043328
            ),
        )(inverse_cov, channel_keep_mask, partner_ids, band_starts)
        return jnp.reshape(found, (2, tile_a, tile_b))

    placed = (P("bl", "bp", None), P("bl", None), P("bl", None), P())
    return jax.shard_map(body, mesh=mesh, in_specs=placed, out_specs=P(None, "bp", "bl"), check_vma=False)
```

```python
from functools import partial

import jax
import jax.numpy as jnp
from jax import lax
from jax.experimental import pallas as pl
from jax.experimental.pallas import tpu as pltpu
from jax.sharding import PartitionSpec as P

WINDOW_LENGTH = 128
KINDS = 4
LANES = 128
PAD = 8
LATE = 2
MESH = pl.DeviceIdType.MESH
NT = (((1,), (1,)), ((), ()))
NN = (((1,), (0,)), ((), ()))
F32, BF16 = jnp.float32, jnp.bfloat16


def split(value):
    high = value.astype(BF16)
    return high, (value - high.astype(F32)).astype(BF16)


def dot(left, right, dims):
    return lax.dot_general(left, right, dims, preferred_element_type=F32)


def dot3(left, right, dims):
    return dot(left[0], right[0], dims) + (dot(left[0], right[1], dims) + dot(left[1], right[0], dims))


def exact(left, right, dims):
    return lax.dot_general(left, right, dims, precision=lax.Precision.HIGHEST, preferred_element_type=F32)


def iota(shape, axis):
    return lax.broadcasted_iota(jnp.int32, shape, axis)


def column_of(row, length, offset):
    shape = (length, row.shape[1])
    spot = iota(shape, 0) + offset == iota(shape, 1)
    return jnp.sum(jnp.where(spot, row, 0.0), axis=1, keepdims=True)


def decay(gap, inverse_length):
    return jnp.exp(-jnp.abs(gap) * inverse_length)


def inverse_of(ids):
    return 1.0 / (1.0 + (ids % KINDS).astype(F32))


def flipped(index, distance):
    result, bit = index, 1
    while bit <= distance:
        if distance & bit:
            result = result + bit - 2 * bit * (index // bit % 2)
        bit *= 2
    return result


def ordered(groups):
    bits = (groups // 2).bit_length() - 1
    far = [d for d in range(1, groups) if bin(d // 2).count("1") == bits]
    direct = [d for d in range(2, groups) if d not in far]
    late = direct[1::2] if len(direct) == 2 * LATE else direct[-LATE:]
    return [d for d in direct if d not in late], far, late


def kernel(
    sizes, cov_ref, mask_ref, partner_ref, starts_ref, out_ref,
    raw, masks, partner_row, starts,
    slices, mask_all, partner_all, rim, rim_out,
    toep, toep_low, table, table_low, spread, spread_low, box, pick,
    held, boxed, leak, blended, mixed, summits, grown, product, tiles, landed,
    load_sem, x_sem, m_sem, p_sem, c_sem, fin_sem, ready, ready_levels,
):
    groups, owners, rows, width, bands, seats = sizes
    window = WINDOW_LENGTH
    me, level = lax.axis_index("bl"), lax.axis_index("bp")
    per_half = width // rows
    half, place = level // per_half, level % per_half
    slots = per_half * groups
    count = rows // groups
    share = bands // slots
    slot = place * groups + me
    first = pl.multiple_of(place * rows, rows)
    mine = pl.ds(first, rows)
    other = pl.ds(pl.multiple_of(width - rows - first, rows), rows)
    half_columns = pl.ds(pl.multiple_of(half * width, width), width)
    early, far, late = ordered(groups)
    arrivals = [0, 1] + far + early + late
    seat_of = {d: n for n, d in enumerate(arrivals)}
    others = far + early + late + [1]
    fixed = groups - LATE
    peers = {d: flipped(me, d) for d in range(groups)}
    levels = {dz: flipped(level, dz) for dz in range(owners)}
    below, above = level > 0, level < owners - 1
    neighbours = below.astype(jnp.int32) + above.astype(jnp.int32)

    starts_load = pltpu.make_async_copy(starts_ref, starts, load_sem.at[2])
    loads = [
        pltpu.make_async_copy(cov_ref.at[0, :, half_columns], raw, load_sem.at[0]),
        pltpu.make_async_copy(mask_ref, masks, load_sem.at[1]),
        pltpu.make_async_copy(partner_ref, partner_row, load_sem.at[3]),
    ]
    starts_load.start()
    for load in loads:
        load.start()

    def tell(semaphore, device):
        pl.semaphore_signal(semaphore, inc=1, device_id=device, device_id_type=MESH)

    def tell_levels(semaphore):
        @pl.when(below)
        def _():
            tell(semaphore, (me, level - 1))

        @pl.when(above)
        def _():
            tell(semaphore, (me, level + 1))

    barrier = pltpu.get_barrier_semaphore()
    for d in others:
        tell(barrier, (peers[d], level))
    tell_levels(barrier)

    def remote(source, target, sems, n, device, shared=False):
        return pltpu.make_async_remote_copy(
            src_ref=source, dst_ref=target, send_sem=sems.at[0, 0 if shared else n], recv_sem=sems.at[1, n],
            device_id=device, device_id_type=MESH,
        )

    def send_marks(d):
        n = seat_of[d]
        remote(partner_row, partner_all.at[n], p_sem, 0, (peers[d], level)).start()
        remote(masks, mask_all.at[n], m_sem, n, (peers[d], level), True).start()

    def send_slice(d):
        n, g = seat_of[d], peers[d]
        part = raw.at[pl.ds(pl.multiple_of(g * count, count), count)]
        remote(part, slices.at[n], x_sem, n, (g, level), True).start()

    def send_rim(d, across):
        n, g = seat_of[d], peers[d]
        row = per_half - 1 - place if across else place
        remote(rim_out.at[row * groups + g], rim.at[n, :, mine], c_sem, across, (g, levels[across])).start()

    def landing(target, sems, n, device):
        remote(target, target, sems, n, device).wait_recv()

    starts_load.wait()
    start_row = starts[pl.ds(half, 1), :].astype(F32)
    start = column_of(start_row, bands, 0)
    band_ids = iota((bands, 1), 0)
    inverse_length = inverse_of(band_ids)
    channel = iota((bands, width), 1).astype(F32)
    ahead = channel - start
    within = jnp.logical_and(ahead >= 0.0, ahead <= window - 1.0)
    rise = decay(ahead, inverse_length)
    fence_ids = iota((slots * KINDS, 1), 0)
    fence_gap = (fence_ids // KINDS * count - 1).astype(F32) - iota((slots * KINDS, width), 1).astype(F32)
    fence = jnp.where(fence_gap >= 0.0, decay(fence_gap, inverse_of(fence_ids)), 0.0)
    sources = split(jnp.concatenate(
        [fence, jnp.where(ahead < 0.0, rise, 0.0), jnp.where(within, rise, 0.0)], axis=0))

    for load in loads:
        load.wait()
    pl.semaphore_wait(barrier, groups - 1 + neighbours)
    tell_levels(ready_levels)
    for d in others:
        send_marks(d)
    for d in others:
        send_slice(d)
    slices[0] = raw[pl.ds(pl.multiple_of(me * count, count), count), :]
    mask_all[0] = masks[...]
    partner_all[0] = partner_row[...]

    marks = masks[:, half_columns].astype(F32)
    panel = split(raw[...] * column_of(marks, rows, first) * marks)
    summed = dot3(sources, panel, NT)
    fences, ups, rises = summed[:slots * KINDS], summed[slots * KINDS:slots * KINDS + bands], summed[slots * KINDS + bands:]
    if share < KINDS:
        rim_out[...] = jnp.zeros_like(rim_out)
    for s in range(slots):
        rim_out[s, 0:KINDS, :] = fences[s * KINDS:(s + 1) * KINDS]
        rim_out[s, KINDS:KINDS + share, :] = ups[s * share:(s + 1) * share]
        rim_out[s, PAD:PAD + share, :] = rises[s * share:(s + 1) * share]
    rim[0, :, mine] = rim_out[slot]
    def ladder(shape, axis):
        return iota(shape, axis).astype(F32)

    twice = jnp.concatenate([start_row, start_row], axis=1)
    pair_ids = iota((1, 2 * bands), 1)
    is_second = iota((width, 2 * bands), 1) >= bands
    pair_inverse = inverse_of(pair_ids)
    climb = ladder((width, 2 * bands), 0) - twice
    drop = climb - (window - 1.0)
    gap = jnp.where(is_second, drop, climb)
    fade = decay(gap, pair_inverse)
    inner = jnp.logical_and(climb >= 0.0, drop <= 0.0)
    outer = jnp.where(is_second, gap, -gap) > 0.0
    mid_ids = iota((1, LANES), 1)
    mid_channel = ladder((width, LANES), 0) - rows
    mid_lane = iota((width, LANES), 1)
    mid_gap = jnp.where(mid_lane < KINDS, -1.0 - mid_channel, mid_channel)
    mid_kept = jnp.logical_and(mid_gap >= 0.0, mid_lane < 2 * KINDS)
    table[...], table_low[...] = split(jnp.concatenate([
        jnp.where(outer, fade, 0.0), jnp.where(inner, fade, 0.0),
        jnp.where(mid_kept, decay(mid_gap, inverse_of(mid_ids)), 0.0)], axis=1))
    far_apart = (iota((rows, rows), 0) - iota((rows, rows), 1)).astype(F32)
    for k in range(KINDS):
        toep[k], toep_low[k] = split(decay(far_apart, 1.0 / (1 + k)))

    pl.semaphore_wait(ready_levels, neighbours)
    for d in range(1, groups):
        tell(ready, (peers[d], level))
    for d in others:
        send_rim(d, 0)

    lane_f = iota((1, rows), 1).astype(F32)
    wide = width + 2 * bands

    def filtered(value):
        n = value.shape[0]
        found = dot3(split(value), (table[...], table_low[...]), NN)
        stacked = split(jnp.concatenate([value[:, 0:rows], value[:, rows:]], axis=0))
        both = jnp.concatenate(stacked, axis=0)
        results = []
        for k in range(KINDS):
            r = dot(both, toep[k], NN)
            r = r[0:2 * n] + r[2 * n:] + dot(stacked[0], toep_low[k], NN)
            up = found[:, 4 * bands + k:4 * bands + k + 1]
            down = found[:, 4 * bands + KINDS + k:4 * bands + KINDS + k + 1]
            left = r[0:n] + down * jnp.exp((rows - lane_f) * (-1.0 / (1 + k)))
            right = r[n:] + up * jnp.exp((lane_f + 1.0) * (-1.0 / (1 + k)))
            results.append((left, right))
        return found[:, 0:2 * bands], found[:, 2 * bands:4 * bands], results

    in_lane = slot * count
    lane_base = pl.multiple_of(half * width + in_lane // LANES * LANES, LANES)
    lane_offset = in_lane % LANES

    def absorb(members):
        parts = []
        for n in members:
            near_marks = mask_all[n, :, pl.ds(lane_base, LANES)].astype(F32)
            part = slices[n] * column_of(near_marks, count, lane_offset) * mask_all[n, :, half_columns].astype(F32)
            held[n, :, 0:width] = part
            parts.append(part)
        edges, ramps, results = filtered(jnp.concatenate(parts, axis=0))
        for i, n in enumerate(members):
            at = slice(i * count, (i + 1) * count)
            leak[n] = edges[at]
            for k in range(KINDS):
                boxed[k, n, :, 0:rows] = results[k][0][at]
                boxed[k, n, :, rows:] = results[k][1][at]
            held[n, :, width:] = ramps[at]

    def take(n):
        device = (peers[arrivals[n]], level)
        landing(mask_all.at[n], m_sem, n, device)
        landing(slices.at[n], x_sem, n, device)

    take(1)
    absorb([0, 1])
    for k in range(KINDS):
        box[:, k * width:(k + 1) * width] = jnp.where(
            jnp.logical_and(within, band_ids % KINDS == k), 1.0, 0.0).astype(BF16)
    sides = iota((bands, 2 * bands), 1) % bands == iota((bands, 2 * bands), 0)
    box[:, KINDS * width:] = jnp.where(sides, -1.0, 0.0).astype(BF16)

    tile_b, tile_a = bands // groups, bands // owners
    span = tile_a * tile_b
    lanes = owners * span
    lane_band = iota((bands, lanes), 1) // tile_b
    lane_start = exact(start_row, (lane_band == iota((bands, lanes), 0)).astype(F32), NN)
    step_rows = KINDS * count
    row_ids = iota((step_rows, lanes), 0)
    row_ahead = (row_ids % count + slot * count).astype(F32) - lane_start
    inside = jnp.logical_and(row_ahead >= 0.0, row_ahead <= window - 1.0)
    of_kind = iota((step_rows, lanes), 1) // tile_b % KINDS == row_ids // count
    pick[0:step_rows, :] = jnp.where(jnp.logical_and(inside, of_kind), 1.0, 0.0)
    rim_row = iota((PAD, lanes), 0)
    own_band = jnp.logical_and(iota((PAD, lanes), 1) // tile_b == slot * share + rim_row - KINDS, rim_row >= KINDS)
    pick[step_rows:, :] = jnp.where(jnp.logical_and(own_band, rim_row < KINDS + share), -1.0, 0.0)

    pl.semaphore_wait(ready, groups - 1)
    for d in others + [0]:
        send_rim(d, 1)

    partners = remote(partner_all.at[1:groups], partner_all.at[1:groups], p_sem, 0, (peers[1], level))
    partners.wait_send()
    partners.wait_recv()
    names = [peers[d] for d in arrivals]
    total = fixed * count
    lane_of, lane_pad = iota((1, total), 1) // count, iota((1, groups * PAD), 1) // PAD
    chosen = [[partner_all[n][:, k:k + 1] for n in range(groups)] for k in range(seats)]

    def along(lane, values):
        found = jnp.zeros_like(lane)
        for n, value in enumerate(values):
            found = jnp.where(lane == n, value, found)
        return found

    named_lane, named_pad = along(lane_of, names[:fixed]), along(lane_pad, names)
    chosen_lane = [along(lane_of, chosen[k][:fixed]) for k in range(seats)]
    chosen_pad = [along(lane_pad, chosen[k]) for k in range(seats)]

    def weights(n, named, by_lane):
        found = 0.0
        for k in range(seats):
            found = found + jnp.where(named == chosen[k][n], 1.0, 0.0) + jnp.where(by_lane[k] == names[n], 1.0, 0.0)
        return found

    def weight(n, i):
        found = 0.0
        for k in range(seats):
            found = found + jnp.where(chosen[k][n] == names[i], 1.0, 0.0) + jnp.where(chosen[k][i] == names[n], 1.0, 0.0)
        return found

    step_gap = (iota((step_rows, total), 0) % count - iota((step_rows, total), 1) % count).astype(F32)
    reach = decay(step_gap, inverse_of(iota((step_rows, total), 0) // count))
    reach = jnp.where(step_gap > 0.0, reach, jnp.where(step_gap == 0.0, 0.5, 0.0))
    blend_rows = []
    pad_row = iota((PAD, groups * PAD), 0)
    slot_lane = jnp.logical_and(
        iota((PAD, groups * PAD), 1) % PAD == pad_row,
        jnp.logical_or(pad_row >= KINDS, iota((PAD, groups * PAD), 1) // PAD < fixed))
    for n in range(groups):
        spread[n], spread_low[n] = split(reach * weights(n, named_lane, chosen_lane))
        blend_rows.append(jnp.where(slot_lane, weights(n, named_pad, chosen_pad), 0.0))
    blend = jnp.concatenate(blend_rows, axis=0).astype(BF16)
    reach_one = split(reach[:, 0:count])

    for n in range(2, fixed, 2):
        for i in (n, n + 1):
            take(i)
        absorb([n, n + 1])

    held_split = split(jnp.reshape(held[0:fixed], (total, wide)))
    for n in range(groups):
        grown[n] = dot3((spread[n], spread_low[n]), held_split, NN)

    members = list(range(fixed, groups))
    for t in range(LATE):
        factors = [weight(fixed + t, n) for n in range(fixed)]
        leak[groups + t] = sum(factors[n] * leak[n] for n in range(fixed))
        for k in range(KINDS):
            blended[k, t] = sum(factors[n] * boxed[k, n] for n in range(fixed))
    for n in members:
        take(n)
    absorb(members)
    for t in range(LATE):
        n = fixed + t
        grown[groups + t] = dot3(reach_one, split(held[n]), NN)
        mutual = weight(n, fixed + 1 - t)
        leak[groups + t] = leak[groups + t] + mutual * leak[fixed + 1 - t]
        for k in range(KINDS):
            blended[k, t] = blended[k, t] + mutual * boxed[k, fixed + 1 - t]

    for target, sems in ((slices, x_sem), (mask_all, m_sem)):
        remote(target.at[1:groups], target.at[1:groups], sems, 0, (peers[1], level)).wait_send()
    for across, columns in ((0, mine), (1, other)):
        ends = rim.at[1 - across:groups, :, columns]
        rims = remote(rim_out.at[1 - across:groups], ends, c_sem, across, (peers[1], levels[across]))
        rims.wait_send()
        rims.wait_recv()
    blank = jnp.zeros((KINDS, width), F32)
    tops, tails = [], []
    for n in range(groups):
        tops.append(rim[n, 0:PAD, :])
        tails += [blank, rim[n, PAD:PAD + share, :]]
        if share < KINDS:
            tails.append(jnp.zeros((KINDS - share, width), F32))
    tops = jnp.concatenate(tops, axis=0)
    tail_edges, _, tail_results = filtered(jnp.concatenate(tails, axis=0))
    tops = jnp.concatenate([tops, dot3(split(tops), (table[:, 2 * bands:4 * bands], table_low[:, 2 * bands:4 * bands]), NN)], axis=1)
    summits[...] = tops
    high, low = split(tops)
    mixed[...] = dot(blend, high, NN) + dot(blend, low, NN)
    rank = (iota((count, 1), 0) + 1).astype(F32)
    fades = [jnp.exp(rank * (-1.0 / (1 + m))) for m in range(KINDS)]
    for k in range(KINDS):
        line = jnp.concatenate(tail_results[k], axis=1)
        product[step_rows:, k * width:(k + 1) * width] = sum(
            mixed[n * PAD:(n + 1) * PAD, 0:width] * line[n * PAD:(n + 1) * PAD] for n in range(groups))
    product[step_rows:, KINDS * width:] = sum(
        mixed[n * PAD:(n + 1) * PAD, width:] * tail_edges[n * PAD:(n + 1) * PAD] for n in range(groups))

    def gather(terms):
        for pb in range(count // 8):
            here = slice(pb * 8, pb * 8 + 8)
            spots = [slice(m * count + pb * 8, m * count + pb * 8 + 8) for m in range(KINDS)]
            for m in range(KINDS):
                found = sum((grown[n, spots[m], width:] + fades[m][here] * carry(m)[:, width:]) * edge[here, :] for n, edge, _, carry in terms)
                at = (spots[m], slice(KINDS * width, wide + (KINDS - 1) * width))
                product[at] = found
            for qb in range(width // LANES):
                cols = slice(qb * LANES, (qb + 1) * LANES)
                sums = [[None] * KINDS for _ in range(KINDS)]
                for n, _, box_ref, carry in terms:
                    lefts = [grown[n, spots[m], cols] + fades[m][here] * carry(m)[:, cols] for m in range(KINDS)]
                    rights = [box_ref(k)[here, cols] for k in range(KINDS)]
                    for m in range(KINDS):
                        for k in range(KINDS):
                            term = lefts[m] * rights[k]
                            sums[m][k] = term if sums[m][k] is None else sums[m][k] + term
                for m in range(KINDS):
                    for k in range(KINDS):
                        at = (spots[m], slice(k * width + qb * LANES, k * width + (qb + 1) * LANES))
                        product[at] = sums[m][k]

    def mixed_carry(n, m):
        return mixed.at[n * PAD + m:n * PAD + m + 1, :]

    def own_carry(n, m):
        return summits.at[n * PAD + m:n * PAD + m + 1, :]

    terms = [(n, leak.at[n], partial(lambda n, k: boxed.at[k, n], n), partial(mixed_carry, n)) for n in range(groups)]
    terms += [
        (groups + t, leak.at[groups + t], partial(lambda t, k: blended.at[k, t], t), partial(own_carry, fixed + t))
        for t in range(LATE)
    ]
    gather(terms)

    high, low = split(product[...])
    turned = split(dot(box[...], high, NT) + dot(box[...], low, NT))
    picks = pick[...].astype(BF16)
    fisher = (dot(turned[0], picks, NN) + dot(turned[1], picks, NN)) * (1.0 / (4 * groups * window))
    kept = jnp.where(iota((bands, lanes), 0) % tile_b == iota((bands, lanes), 1) % tile_b, fisher, 0.0)
    for g in range(groups):
        packed = jnp.sum(kept[g * tile_b:(g + 1) * tile_b], axis=0, keepdims=True)
        for z in range(owners):
            tiles[z * groups + g] = packed[:, z * span:(z + 1) * span]

    landed[0] = tiles[level * groups + me]
    everyone = groups * owners
    for dz in reversed(range(owners)):
        for d in others + [0]:
            if dz or d:
                n = dz * groups + d
                remote(
                    tiles.at[levels[dz] * groups + peers[d]], landed.at[n], fin_sem, 0, (peers[d], levels[dz])).start()
    finals = remote(tiles.at[1:everyone], landed.at[1:everyone], fin_sem, 0, (peers[1], level))
    finals.wait_send()
    finals.wait_recv()
    for side in range(2):
        part = landed[side * per_half * groups:(side + 1) * per_half * groups]
        out_ref[pl.ds(half + side - 2 * side * half, 1), :] = jnp.sum(part, axis=0)


def solution(mesh):
    groups, owners = mesh.shape["bl"], mesh.shape["bp"]

    def body(inverse_cov, channel_keep_mask, partner_ids, band_starts):
        number, rows, channels = inverse_cov.shape
        width, bands, seats = channels // 2, band_starts.shape[1], partner_ids.shape[1]
        per_half = width // rows
        slots = per_half * groups
        count, share = rows // groups, bands // slots
        assert number == 1 and per_half == 2 and owners == 4 and count % 8 == 0 and 1 <= share <= KINDS
        tile_b, tile_a = bands // groups, bands // owners
        wide = width + 2 * bands
        step_rows = KINDS * count
        everyone = groups * owners
        dma = pltpu.SemaphoreType.DMA
        regular = pltpu.SemaphoreType.REGULAR

        def vmem(shape, dtype=F32):
            return pltpu.VMEM(shape, dtype)

        found = pl.pallas_call(
            partial(kernel, (groups, owners, rows, width, bands, seats)),
            name="fisher",
            out_shape=jax.ShapeDtypeStruct((2, tile_a * tile_b), F32),
            in_specs=[pl.BlockSpec(memory_space=pltpu.HBM)] * 4,
            out_specs=pl.BlockSpec(memory_space=pltpu.VMEM),
            scratch_shapes=[
                vmem((rows, width)),
                vmem(channel_keep_mask.shape, jnp.int32),
                vmem(partner_ids.shape, jnp.int32),
                vmem(band_starts.shape, jnp.int32),
                vmem((groups, count, width)),
                vmem((groups, 1, channels), jnp.int32),
                vmem((groups, 1, seats), jnp.int32),
                vmem((groups, PAD + share, width)),
                vmem((slots, PAD + share, rows)),
                vmem((KINDS, rows, rows), BF16),
                vmem((KINDS, rows, rows), BF16),
                vmem((width, 4 * bands + LANES), BF16),
                vmem((width, 4 * bands + LANES), BF16),
                vmem((groups, step_rows, (groups - LATE) * count), BF16),
                vmem((groups, step_rows, (groups - LATE) * count), BF16),
                vmem((bands, KINDS * width + 2 * bands), BF16),
                vmem((step_rows + PAD, bands * tile_b)),
                vmem((groups, count, wide)),
                vmem((KINDS, groups, count, width)),
                vmem((groups + LATE, count, 2 * bands)),
                vmem((KINDS, LATE, count, width)),
                vmem((groups * PAD, wide)),
                vmem((groups * PAD, wide)),
                vmem((groups + LATE, step_rows, wide)),
                vmem((step_rows + PAD, KINDS * width + 2 * bands)),
                vmem((everyone, 1, tile_a * tile_b)),
                vmem((everyone, 1, tile_a * tile_b)),
                dma((4,)), dma((2, groups)), dma((2, groups)), dma((2, 1)), dma((2, per_half)),
                dma((2, 1)), regular, regular,
            ],
            compiler_params=pltpu.CompilerParams(
                collective_id=0, has_side_effects=True, vmem_limit_bytes=67043328
            ),
        )(inverse_cov, channel_keep_mask, partner_ids, band_starts)
        return jnp.reshape(found, (2, tile_a, tile_b))

    placed = (P("bl", "bp", None), P("bl", None), P("bl", None), P())
    return jax.shard_map(body, mesh=mesh, in_specs=placed, out_specs=P(None, "bp", "bl"), check_vma=False)
```

```python
from functools import partial

import jax
import jax.numpy as jnp
from jax import lax
from jax.experimental import pallas as pl
from jax.experimental.pallas import tpu as pltpu
from jax.sharding import PartitionSpec as P

WINDOW_LENGTH = 128
KINDS = 4
LANES = 128
PAD = 8
LATE = 2
MESH = pl.DeviceIdType.MESH
NT = (((1,), (1,)), ((), ()))
NN = (((1,), (0,)), ((), ()))
F32, BF16 = jnp.float32, jnp.bfloat16


def split(value):
    high = value.astype(BF16)
    return high, (value - high.astype(F32)).astype(BF16)


def dot(left, right, dims):
    return lax.dot_general(left, right, dims, preferred_element_type=F32)


def dot3(left, right, dims):
    return dot(left[0], right[0], dims) + (dot(left[0], right[1], dims) + dot(left[1], right[0], dims))


def stacked3(left, right):
    rows = left[0].shape[0]
    pairs = dot(jnp.concatenate(left, axis=0), right[0], NN)
    return pairs[0:rows] + pairs[rows:] + dot(left[0], right[1], NN)


def exact(left, right, dims):
    return lax.dot_general(left, right, dims, precision=lax.Precision.HIGHEST, preferred_element_type=F32)


def iota(shape, axis):
    return lax.broadcasted_iota(jnp.int32, shape, axis)


def column_of(row, length, offset):
    shape = (length, row.shape[1])
    spot = iota(shape, 0) + offset == iota(shape, 1)
    return jnp.sum(jnp.where(spot, row, 0.0), axis=1, keepdims=True)


def decay(gap, inverse_length):
    return jnp.exp(-jnp.abs(gap) * inverse_length)


def inverse_of(ids):
    return 1.0 / (1.0 + (ids % KINDS).astype(F32))


def flipped(index, distance):
    result, bit = index, 1
    while bit <= distance:
        if distance & bit:
            result = result + bit - 2 * bit * (index // bit % 2)
        bit *= 2
    return result


def ordered(groups):
    bits = (groups // 2).bit_length() - 1
    far = [d for d in range(1, groups) if bin(d // 2).count("1") == bits]
    direct = [d for d in range(2, groups) if d not in far]
    late = direct[1::2] if len(direct) == 2 * LATE else direct[-LATE:]
    return [d for d in direct if d not in late], far, late


def kernel(
    sizes, cov_ref, mask_ref, partner_ref, starts_ref, out_ref,
    raw, masks, partner_row, starts,
    slices, mask_all, partner_all, rim, rim_out,
    toep, toep_low, table, table_low, spread, spread_low, box, pick,
    held, boxed, leak, blended, mixed, summits, grown, product, tiles, landed,
    load_sem, x_sem, m_sem, p_sem, c_sem, fin_sem, ready, ready_levels,
):
    groups, owners, rows, width, bands, seats = sizes
    window = WINDOW_LENGTH
    me, level = lax.axis_index("bl"), lax.axis_index("bp")
    per_half = width // rows
    half, place = level // per_half, level % per_half
    slots = per_half * groups
    count = rows // groups
    share = bands // slots
    slot = place * groups + me
    first = pl.multiple_of(place * rows, rows)
    mine = pl.ds(first, rows)
    other = pl.ds(pl.multiple_of(width - rows - first, rows), rows)
    half_columns = pl.ds(pl.multiple_of(half * width, width), width)
    early, far, late = ordered(groups)
    arrivals = [0, 1] + far + early + late
    seat_of = {d: n for n, d in enumerate(arrivals)}
    others = far + early + late + [1]
    fixed = groups - LATE
    peers = {d: flipped(me, d) for d in range(groups)}
    levels = {dz: flipped(level, dz) for dz in range(owners)}
    below, above = level > 0, level < owners - 1
    neighbours = below.astype(jnp.int32) + above.astype(jnp.int32)

    starts_load = pltpu.make_async_copy(starts_ref, starts, load_sem.at[2])
    loads = [
        pltpu.make_async_copy(cov_ref.at[0, :, half_columns], raw, load_sem.at[0]),
        pltpu.make_async_copy(mask_ref, masks, load_sem.at[1]),
        pltpu.make_async_copy(partner_ref, partner_row, load_sem.at[3]),
    ]
    starts_load.start()
    for load in loads:
        load.start()

    def tell(semaphore, device):
        pl.semaphore_signal(semaphore, inc=1, device_id=device, device_id_type=MESH)

    def tell_levels(semaphore):
        @pl.when(below)
        def _():
            tell(semaphore, (me, level - 1))

        @pl.when(above)
        def _():
            tell(semaphore, (me, level + 1))

    barrier = pltpu.get_barrier_semaphore()
    for d in others:
        tell(barrier, (peers[d], level))
    tell_levels(barrier)

    def remote(source, target, sems, n, device, shared=False):
        return pltpu.make_async_remote_copy(
            src_ref=source, dst_ref=target, send_sem=sems.at[0, 0 if shared else n], recv_sem=sems.at[1, n],
            device_id=device, device_id_type=MESH,
        )

    def send_marks(d):
        n = seat_of[d]
        remote(partner_row, partner_all.at[n], p_sem, 0, (peers[d], level)).start()
        remote(masks, mask_all.at[n], m_sem, n, (peers[d], level), True).start()

    def send_slice(d):
        n, g = seat_of[d], peers[d]
        part = raw.at[pl.ds(pl.multiple_of(g * count, count), count)]
        remote(part, slices.at[n], x_sem, n, (g, level), True).start()

    def send_rim(d, across):
        n, g = seat_of[d], peers[d]
        row = per_half - 1 - place if across else place
        remote(rim_out.at[row * groups + g], rim.at[n, :, mine], c_sem, across, (g, levels[across])).start()

    def landing(target, sems, n, device):
        remote(target, target, sems, n, device).wait_recv()

    starts_load.wait()
    start_row = starts[pl.ds(half, 1), :].astype(F32)
    start = column_of(start_row, bands, 0)
    band_ids = iota((bands, 1), 0)
    inverse_length = inverse_of(band_ids)
    channel = iota((bands, width), 1).astype(F32)
    ahead = channel - start
    within = jnp.logical_and(ahead >= 0.0, ahead <= window - 1.0)
    rise = decay(ahead, inverse_length)
    fence_ids = iota((slots * KINDS, 1), 0)
    fence_gap = (fence_ids // KINDS * count - 1).astype(F32) - iota((slots * KINDS, width), 1).astype(F32)
    fence = jnp.where(fence_gap >= 0.0, decay(fence_gap, inverse_of(fence_ids)), 0.0)
    sources = split(jnp.concatenate(
        [fence, jnp.where(ahead < 0.0, rise, 0.0), jnp.where(within, rise, 0.0)], axis=0))

    for load in loads:
        load.wait()
    pl.semaphore_wait(barrier, groups - 1 + neighbours)
    tell_levels(ready_levels)
    for d in others:
        send_marks(d)
    for d in others:
        send_slice(d)
    slices[0] = raw[pl.ds(pl.multiple_of(me * count, count), count), :]
    mask_all[0] = masks[...]
    partner_all[0] = partner_row[...]

    marks = masks[:, half_columns].astype(F32)
    panel = split(raw[...] * column_of(marks, rows, first) * marks)
    summed = dot3(sources, panel, NT)
    fences, ups, rises = summed[:slots * KINDS], summed[slots * KINDS:slots * KINDS + bands], summed[slots * KINDS + bands:]
    if share < KINDS:
        rim_out[...] = jnp.zeros_like(rim_out)
    for s in range(slots):
        rim_out[s, 0:KINDS, :] = fences[s * KINDS:(s + 1) * KINDS]
        rim_out[s, KINDS:KINDS + share, :] = ups[s * share:(s + 1) * share]
        rim_out[s, PAD:PAD + share, :] = rises[s * share:(s + 1) * share]
    rim[0, :, mine] = rim_out[slot]
    def ladder(shape, axis):
        return iota(shape, axis).astype(F32)

    twice = jnp.concatenate([start_row, start_row], axis=1)
    pair_ids = iota((1, 2 * bands), 1)
    is_second = iota((width, 2 * bands), 1) >= bands
    pair_inverse = inverse_of(pair_ids)
    climb = ladder((width, 2 * bands), 0) - twice
    drop = climb - (window - 1.0)
    gap = jnp.where(is_second, drop, climb)
    fade = decay(gap, pair_inverse)
    inner = jnp.logical_and(climb >= 0.0, drop <= 0.0)
    outer = jnp.where(is_second, gap, -gap) > 0.0
    mid_ids = iota((1, LANES), 1)
    mid_channel = ladder((width, LANES), 0) - rows
    mid_lane = iota((width, LANES), 1)
    mid_gap = jnp.where(mid_lane < KINDS, -1.0 - mid_channel, mid_channel)
    mid_kept = jnp.logical_and(mid_gap >= 0.0, mid_lane < 2 * KINDS)
    table[...], table_low[...] = split(jnp.concatenate([
        jnp.where(outer, fade, 0.0), jnp.where(inner, fade, 0.0),
        jnp.where(mid_kept, decay(mid_gap, inverse_of(mid_ids)), 0.0)], axis=1))
    far_apart = (iota((rows, rows), 0) - iota((rows, rows), 1)).astype(F32)
    for k in range(KINDS):
        toep[k], toep_low[k] = split(decay(far_apart, 1.0 / (1 + k)))

    pl.semaphore_wait(ready_levels, neighbours)
    for d in range(1, groups):
        tell(ready, (peers[d], level))
    for d in others:
        send_rim(d, 0)

    lane_f = iota((1, rows), 1).astype(F32)
    wide = width + 2 * bands

    def filtered(value):
        n = value.shape[0]
        found = stacked3(split(value), (table[...], table_low[...]))
        stacked = split(jnp.concatenate([value[:, 0:rows], value[:, rows:]], axis=0))
        both = jnp.concatenate(stacked, axis=0)
        results = []
        for k in range(KINDS):
            r = dot(both, toep[k], NN)
            r = r[0:2 * n] + r[2 * n:] + dot(stacked[0], toep_low[k], NN)
            up = found[:, 4 * bands + k:4 * bands + k + 1]
            down = found[:, 4 * bands + KINDS + k:4 * bands + KINDS + k + 1]
            left = r[0:n] + down * jnp.exp((rows - lane_f) * (-1.0 / (1 + k)))
            right = r[n:] + up * jnp.exp((lane_f + 1.0) * (-1.0 / (1 + k)))
            results.append((left, right))
        return found[:, 0:2 * bands], found[:, 2 * bands:4 * bands], results

    in_lane = slot * count
    lane_base = pl.multiple_of(half * width + in_lane // LANES * LANES, LANES)
    lane_offset = in_lane % LANES

    def absorb(members):
        parts = []
        for n in members:
            near_marks = mask_all[n, :, pl.ds(lane_base, LANES)].astype(F32)
            part = slices[n] * column_of(near_marks, count, lane_offset) * mask_all[n, :, half_columns].astype(F32)
            held[n, :, 0:width] = part
            parts.append(part)
        edges, ramps, results = filtered(jnp.concatenate(parts, axis=0))
        for i, n in enumerate(members):
            at = slice(i * count, (i + 1) * count)
            leak[n] = edges[at]
            for k in range(KINDS):
                boxed[k, n, :, 0:rows] = results[k][0][at]
                boxed[k, n, :, rows:] = results[k][1][at]
            held[n, :, width:] = ramps[at]

    def take(n):
        device = (peers[arrivals[n]], level)
        landing(mask_all.at[n], m_sem, n, device)
        landing(slices.at[n], x_sem, n, device)

    take(1)
    absorb([0, 1])
    for k in range(KINDS):
        box[:, k * width:(k + 1) * width] = jnp.where(
            jnp.logical_and(within, band_ids % KINDS == k), 1.0, 0.0).astype(BF16)
    sides = iota((bands, 2 * bands), 1) % bands == iota((bands, 2 * bands), 0)
    box[:, KINDS * width:] = jnp.where(sides, -1.0, 0.0).astype(BF16)

    tile_b, tile_a = bands // groups, bands // owners
    span = tile_a * tile_b
    lanes = owners * span
    lane_band = iota((bands, lanes), 1) // tile_b
    lane_start = exact(start_row, (lane_band == iota((bands, lanes), 0)).astype(F32), NN)
    step_rows = KINDS * count
    row_ids = iota((step_rows, lanes), 0)
    row_ahead = (row_ids % count + slot * count).astype(F32) - lane_start
    inside = jnp.logical_and(row_ahead >= 0.0, row_ahead <= window - 1.0)
    of_kind = iota((step_rows, lanes), 1) // tile_b % KINDS == row_ids // count
    pick[0:step_rows, :] = jnp.where(jnp.logical_and(inside, of_kind), 1.0, 0.0)
    rim_row = iota((PAD, lanes), 0)
    own_band = jnp.logical_and(iota((PAD, lanes), 1) // tile_b == slot * share + rim_row - KINDS, rim_row >= KINDS)
    pick[step_rows:, :] = jnp.where(jnp.logical_and(own_band, rim_row < KINDS + share), -1.0, 0.0)

    pl.semaphore_wait(ready, groups - 1)
    for d in others + [0]:
        send_rim(d, 1)

    partners = remote(partner_all.at[1:groups], partner_all.at[1:groups], p_sem, 0, (peers[1], level))
    partners.wait_send()
    partners.wait_recv()
    names = [peers[d] for d in arrivals]
    total = fixed * count
    lane_of, lane_pad = iota((1, total), 1) // count, iota((1, groups * PAD), 1) // PAD
    chosen = [[partner_all[n][:, k:k + 1] for n in range(groups)] for k in range(seats)]

    def along(lane, values):
        found = jnp.zeros_like(lane)
        for n, value in enumerate(values):
            found = jnp.where(lane == n, value, found)
        return found

    named_lane, named_pad = along(lane_of, names[:fixed]), along(lane_pad, names)
    chosen_lane = [along(lane_of, chosen[k][:fixed]) for k in range(seats)]
    chosen_pad = [along(lane_pad, chosen[k]) for k in range(seats)]

    def weights(n, named, by_lane):
        found = 0.0
        for k in range(seats):
            found = found + jnp.where(named == chosen[k][n], 1.0, 0.0) + jnp.where(by_lane[k] == names[n], 1.0, 0.0)
        return found

    def weight(n, i):
        found = 0.0
        for k in range(seats):
            found = found + jnp.where(chosen[k][n] == names[i], 1.0, 0.0) + jnp.where(chosen[k][i] == names[n], 1.0, 0.0)
        return found

    step_gap = (iota((step_rows, total), 0) % count - iota((step_rows, total), 1) % count).astype(F32)
    reach = decay(step_gap, inverse_of(iota((step_rows, total), 0) // count))
    reach = jnp.where(step_gap > 0.0, reach, jnp.where(step_gap == 0.0, 0.5, 0.0))
    blend_rows = []
    pad_row = iota((PAD, groups * PAD), 0)
    slot_lane = jnp.logical_and(
        iota((PAD, groups * PAD), 1) % PAD == pad_row,
        jnp.logical_or(pad_row >= KINDS, iota((PAD, groups * PAD), 1) // PAD < fixed))
    for n in range(groups):
        spread[n], spread_low[n] = split(reach * weights(n, named_lane, chosen_lane))
        blend_rows.append(jnp.where(slot_lane, weights(n, named_pad, chosen_pad), 0.0))
    blend = jnp.concatenate(blend_rows, axis=0).astype(BF16)
    reach_one = split(reach[:, 0:count])

    for n in range(2, fixed, 2):
        for i in (n, n + 1):
            take(i)
        absorb([n, n + 1])

    held_split = split(jnp.reshape(held[0:fixed], (total, wide)))
    for n in range(groups):
        grown[n] = stacked3((spread[n], spread_low[n]), held_split)

    members = list(range(fixed, groups))
    for t in range(LATE):
        factors = [weight(fixed + t, n) for n in range(fixed)]
        leak[groups + t] = sum(factors[n] * leak[n] for n in range(fixed))
        for k in range(KINDS):
            blended[k, t] = sum(factors[n] * boxed[k, n] for n in range(fixed))
    for n in members:
        take(n)
    absorb(members)
    for t in range(LATE):
        n = fixed + t
        grown[groups + t] = stacked3(reach_one, split(held[n]))
        mutual = weight(n, fixed + 1 - t)
        leak[groups + t] = leak[groups + t] + mutual * leak[fixed + 1 - t]
        for k in range(KINDS):
            blended[k, t] = blended[k, t] + mutual * boxed[k, fixed + 1 - t]

    for target, sems in ((slices, x_sem), (mask_all, m_sem)):
        remote(target.at[1:groups], target.at[1:groups], sems, 0, (peers[1], level)).wait_send()
    for across, columns in ((0, mine), (1, other)):
        ends = rim.at[1 - across:groups, :, columns]
        rims = remote(rim_out.at[1 - across:groups], ends, c_sem, across, (peers[1], levels[across]))
        rims.wait_send()
        rims.wait_recv()
    blank = jnp.zeros((KINDS, width), F32)
    tops, tails = [], []
    for n in range(groups):
        tops.append(rim[n, 0:PAD, :])
        tails += [blank, rim[n, PAD:PAD + share, :]]
        if share < KINDS:
            tails.append(jnp.zeros((KINDS - share, width), F32))
    tops = jnp.concatenate(tops, axis=0)
    tail_edges, _, tail_results = filtered(jnp.concatenate(tails, axis=0))
    tops = jnp.concatenate([tops, dot3(split(tops), (table[:, 2 * bands:4 * bands], table_low[:, 2 * bands:4 * bands]), NN)], axis=1)
    summits[...] = tops
    high, low = split(tops)
    mixed[...] = dot(blend, high, NN) + dot(blend, low, NN)
    rank = (iota((count, 1), 0) + 1).astype(F32)
    fades = [jnp.exp(rank * (-1.0 / (1 + m))) for m in range(KINDS)]
    for k in range(KINDS):
        line = jnp.concatenate(tail_results[k], axis=1)
        product[step_rows:, k * width:(k + 1) * width] = sum(
            mixed[n * PAD:(n + 1) * PAD, 0:width] * line[n * PAD:(n + 1) * PAD] for n in range(groups))
    product[step_rows:, KINDS * width:] = sum(
        mixed[n * PAD:(n + 1) * PAD, width:] * tail_edges[n * PAD:(n + 1) * PAD] for n in range(groups))

    def gather(terms):
        for pb in range(count // 8):
            here = slice(pb * 8, pb * 8 + 8)
            spots = [slice(m * count + pb * 8, m * count + pb * 8 + 8) for m in range(KINDS)]
            for m in range(KINDS):
                found = sum((grown[n, spots[m], width:] + fades[m][here] * carry(m)[:, width:]) * edge[here, :] for n, edge, _, carry in terms)
                at = (spots[m], slice(KINDS * width, wide + (KINDS - 1) * width))
                product[at] = found
            for qb in range(width // LANES):
                cols = slice(qb * LANES, (qb + 1) * LANES)
                sums = [[None] * KINDS for _ in range(KINDS)]
                for n, _, box_ref, carry in terms:
                    lefts = [grown[n, spots[m], cols] + fades[m][here] * carry(m)[:, cols] for m in range(KINDS)]
                    rights = [box_ref(k)[here, cols] for k in range(KINDS)]
                    for m in range(KINDS):
                        for k in range(KINDS):
                            term = lefts[m] * rights[k]
                            sums[m][k] = term if sums[m][k] is None else sums[m][k] + term
                for m in range(KINDS):
                    for k in range(KINDS):
                        at = (spots[m], slice(k * width + qb * LANES, k * width + (qb + 1) * LANES))
                        product[at] = sums[m][k]

    def mixed_carry(n, m):
        return mixed.at[n * PAD + m:n * PAD + m + 1, :]

    def own_carry(n, m):
        return summits.at[n * PAD + m:n * PAD + m + 1, :]

    terms = [(n, leak.at[n], partial(lambda n, k: boxed.at[k, n], n), partial(mixed_carry, n)) for n in range(groups)]
    terms += [
        (groups + t, leak.at[groups + t], partial(lambda t, k: blended.at[k, t], t), partial(own_carry, fixed + t))
        for t in range(LATE)
    ]
    gather(terms)

    high, low = split(product[...])
    turned = split(dot(box[...], high, NT) + dot(box[...], low, NT))
    picks = pick[...].astype(BF16)
    fisher = (dot(turned[0], picks, NN) + dot(turned[1], picks, NN)) * (1.0 / (4 * groups * window))
    kept = jnp.where(iota((bands, lanes), 0) % tile_b == iota((bands, lanes), 1) % tile_b, fisher, 0.0)
    for g in range(groups):
        packed = jnp.sum(kept[g * tile_b:(g + 1) * tile_b], axis=0, keepdims=True)
        for z in range(owners):
            tiles[z * groups + g] = packed[:, z * span:(z + 1) * span]

    landed[0] = tiles[level * groups + me]
    everyone = groups * owners
    for dz in reversed(range(owners)):
        for d in others + [0]:
            if dz or d:
                n = dz * groups + d
                remote(
                    tiles.at[levels[dz] * groups + peers[d]], landed.at[n], fin_sem, 0, (peers[d], levels[dz])).start()
    finals = remote(tiles.at[1:everyone], landed.at[1:everyone], fin_sem, 0, (peers[1], level))
    finals.wait_send()
    finals.wait_recv()
    for side in range(2):
        part = landed[side * per_half * groups:(side + 1) * per_half * groups]
        out_ref[pl.ds(half + side - 2 * side * half, 1), :] = jnp.sum(part, axis=0)


def solution(mesh):
    groups, owners = mesh.shape["bl"], mesh.shape["bp"]

    def body(inverse_cov, channel_keep_mask, partner_ids, band_starts):
        number, rows, channels = inverse_cov.shape
        width, bands, seats = channels // 2, band_starts.shape[1], partner_ids.shape[1]
        per_half = width // rows
        slots = per_half * groups
        count, share = rows // groups, bands // slots
        assert number == 1 and per_half == 2 and owners == 4 and count % 8 == 0 and 1 <= share <= KINDS
        tile_b, tile_a = bands // groups, bands // owners
        wide = width + 2 * bands
        step_rows = KINDS * count
        everyone = groups * owners
        dma = pltpu.SemaphoreType.DMA
        regular = pltpu.SemaphoreType.REGULAR

        def vmem(shape, dtype=F32):
            return pltpu.VMEM(shape, dtype)

        found = pl.pallas_call(
            partial(kernel, (groups, owners, rows, width, bands, seats)),
            name="fisher",
            out_shape=jax.ShapeDtypeStruct((2, tile_a * tile_b), F32),
            in_specs=[pl.BlockSpec(memory_space=pltpu.HBM)] * 4,
            out_specs=pl.BlockSpec(memory_space=pltpu.VMEM),
            scratch_shapes=[
                vmem((rows, width)),
                vmem(channel_keep_mask.shape, jnp.int32),
                vmem(partner_ids.shape, jnp.int32),
                vmem(band_starts.shape, jnp.int32),
                vmem((groups, count, width)),
                vmem((groups, 1, channels), jnp.int32),
                vmem((groups, 1, seats), jnp.int32),
                vmem((groups, PAD + share, width)),
                vmem((slots, PAD + share, rows)),
                vmem((KINDS, rows, rows), BF16),
                vmem((KINDS, rows, rows), BF16),
                vmem((width, 4 * bands + LANES), BF16),
                vmem((width, 4 * bands + LANES), BF16),
                vmem((groups, step_rows, (groups - LATE) * count), BF16),
                vmem((groups, step_rows, (groups - LATE) * count), BF16),
                vmem((bands, KINDS * width + 2 * bands), BF16),
                vmem((step_rows + PAD, bands * tile_b)),
                vmem((groups, count, wide)),
                vmem((KINDS, groups, count, width)),
                vmem((groups + LATE, count, 2 * bands)),
                vmem((KINDS, LATE, count, width)),
                vmem((groups * PAD, wide)),
                vmem((groups * PAD, wide)),
                vmem((groups + LATE, step_rows, wide)),
                vmem((step_rows + PAD, KINDS * width + 2 * bands)),
                vmem((everyone, 1, tile_a * tile_b)),
                vmem((everyone, 1, tile_a * tile_b)),
                dma((4,)), dma((2, groups)), dma((2, groups)), dma((2, 1)), dma((2, per_half)),
                dma((2, 1)), regular, regular,
            ],
            compiler_params=pltpu.CompilerParams(
                collective_id=0, has_side_effects=True, vmem_limit_bytes=67043328
            ),
        )(inverse_cov, channel_keep_mask, partner_ids, band_starts)
        return jnp.reshape(found, (2, tile_a, tile_b))

    placed = (P("bl", "bp", None), P("bl", None), P("bl", None), P())
    return jax.shard_map(body, mesh=mesh, in_specs=placed, out_specs=P(None, "bp", "bl"), check_vma=False)
```
